512 devices in a mesh: grp: 2 (over y), row: 32 (over z), col: 4 (over x), frm: 2 (over core).
Axes of the slice: x: 4, y: 2, z: 32, core: 2. Of those that a mesh axis runs over, the one named last changes fastest.
The devices are a block of a 4x8x32 slice.
Arguments:
- latent: bfloat16 [4, 128, 640, 256], P(('grp', 'frm'), 'row', 'col'), parts along dimension 0, may hold values from -6 to 6
- proj_weight: bfloat16 [256, 128], replicated, may hold values from -0.375 to 0.375
- proj_bias: float32 [128], replicated, may hold values from -3 to 3
- cache_one: bfloat16 [4, 256, 1280, 128], P(('grp', 'frm'), 'row', 'col'), parts along dimension 0, may hold values from -6 to 6
- cache_two: bfloat16 [4, 256, 1280, 128], P(('grp', 'frm'), 'row', 'col'), parts along dimension 0, may hold values from -6 to 6
- conv_one: bfloat16 [3, 3, 3, 128, 128], replicated, may hold values from -0.109375 to 0.109375
- bias_one: float32 [128], replicated, may hold values from -3 to 3
- conv_two: bfloat16 [3, 3, 3, 128, 128], replicated, may hold values from -0.109375 to 0.109375
- bias_two: float32 [128], replicated, may hold values from -3 to 3
Outputs:
- decoded: bfloat16 [4, 256, 1280, 128], P(('grp', 'frm'), 'row', 'col'), parts along dimension 0
The draws below stay inside these ranges and needn't reach their ends.
There are 2 independent parts, one for each index of `grp`. The reference program is written for one: setup_inputs(seed, part) draws one part's arguments, and reference() takes and returns one part's arrays. A program takes and returns all parts, laid end to end along the dimension named above; an argument that names none is the same for every part. Nothing has to cross between parts.
All inputs are finite; a program needn't handle non-finite values.
Results may differ from the reference program's by a relative error of at most 0.0044.
Values may be sent and summed in bfloat16 or wider, within the bound.
No kernel may reach another device: no remote copies, remote signals or barrier semaphores. Data moves between devices by JAX's collectives and lax.ppermute only.
A program may use at most 64 MiB of HBM per device.

```python
import jax
import jax.numpy as jnp

LCH = 256
CH = 128
FRAMES = 2
H = 256
W = 1280
LH = 128
LW = 640


def block_scale(rng, extent, shards, least, top_value):
    loudness = 1.0
    for dim, parts in shards:
        steps = jax.random.uniform(jax.random.fold_in(jax.random.fold_in(rng, 6), dim), (parts,), jnp.float32, least / len(shards), top_value / len(shards))
        loudness = loudness * jnp.repeat(jnp.exp(steps), extent[dim] // parts).reshape((-1,) + (1,) * (len(extent) - 1 - dim))
    return loudness


def centred(rng, dims, scale, limit, split=(), dtype=jnp.bfloat16):
    gain = block_scale(rng, dims, split, -0.22, 0.18) if split else 1.0
    values = jax.random.normal(rng, dims, jnp.float32) * scale * gain
    return jnp.minimum(jnp.maximum(values, -limit), limit).astype(dtype)


def setup_inputs(seed: int = 0, part: int = 0) -> dict:
    keys = jax.random.split(jax.random.key(seed), 10)
    own_keys = jax.random.split(jax.random.fold_in(keys[9], part), 10)
    latent = centred(own_keys[0], (FRAMES, LH, LW, LCH), 1.0, 6.0, ((0, 2), (1, 32), (2, 4)))
    proj_weight = centred(keys[1], (LCH, CH), LCH ** -0.5, 0.375)
    proj_bias = centred(keys[2], (CH,), 0.5, 3.0, (), jnp.float32)
    cache_one = centred(own_keys[3], (FRAMES, H, W, CH), 1.0, 6.0, ((0, 2), (1, 32), (2, 4)))
    cache_two = centred(own_keys[4], (FRAMES, H, W, CH), 1.0, 6.0, ((0, 2), (1, 32), (2, 4)))
    conv_one = centred(keys[5], (3, 3, 3, CH, CH), (27 * CH) ** -0.5, 0.109375)
    bias_one = centred(keys[6], (CH,), 0.5, 3.0, (), jnp.float32)
    conv_two = centred(keys[7], (3, 3, 3, CH, CH), (27 * CH) ** -0.5, 0.109375)
    bias_two = centred(keys[8], (CH,), 0.5, 3.0, (), jnp.float32)
    return {"latent": latent, "proj_weight": proj_weight, "proj_bias": proj_bias, "cache_one": cache_one, "cache_two": cache_two, "conv_one": conv_one, "bias_one": bias_one, "conv_two": conv_two, "bias_two": bias_two}


def causal_conv(frames, weight, bias):
    tile_rows, tile_cols, channels = frames.shape[1], frames.shape[2], frames.shape[3]
    padded = jnp.pad(frames, ((0, 0), (1, 1), (1, 1), (0, 0)))
    folded = weight.reshape(3, 3, 3 * channels, weight.shape[-1])
    results = []
    for frame_out in range(frames.shape[0] - 2):
        summed = jnp.zeros((tile_rows * tile_cols, weight.shape[-1]), jnp.float32)
        for frame_step in range(3):
            for row_step in range(3):
                stencil = jnp.concatenate(
                    [padded[frame_out + frame_step, row_step:row_step + tile_rows, col_step:col_step + tile_cols]
                     for col_step in range(3)], axis=-1).reshape(tile_rows * tile_cols, 3 * channels)
                summed = summed + jnp.dot(stencil, folded[frame_step, row_step], preferred_element_type=jnp.float32)
        results.append((summed + bias).reshape(tile_rows, tile_cols, -1))
    return jnp.stack(results)


def reference(latent, proj_weight, proj_bias, cache_one, cache_two, conv_one, bias_one, conv_two, bias_two):
    projected = jnp.dot(latent.reshape(-1, latent.shape[-1]), proj_weight, preferred_element_type=jnp.float32) + proj_bias
    projected = projected.reshape(latent.shape[0], latent.shape[1], latent.shape[2], -1)
    upsampled = jnp.repeat(jnp.repeat(projected.astype(jnp.bfloat16), 2, axis=1), 2, axis=2)
    act_one = jax.nn.silu(upsampled.astype(jnp.float32)).astype(jnp.bfloat16)
    first_out = causal_conv(jnp.concatenate([cache_one, act_one], axis=0), conv_one, bias_one)
    act_two = jax.nn.silu(first_out).astype(jnp.bfloat16)
    second_out = causal_conv(jnp.concatenate([cache_two, act_two], axis=0), conv_two, bias_two)
    return (upsampled.astype(jnp.float32) + second_out).astype(jnp.bfloat16)
```

```python
import functools

import jax
import jax.numpy as jnp
from jax import lax
from jax.experimental import pallas as pl
from jax.experimental.pallas import tpu as pltpu
from jax.sharding import PartitionSpec as P

B = 16
BF = jnp.bfloat16
F32 = jnp.float32
VMEM = pl.BlockSpec(memory_space=pltpu.VMEM)
SMEM = pl.BlockSpec(memory_space=pltpu.SMEM)


def call(body, outs, scratch=(), flops=0, nbytes=0, smem_first=False, n_in=0, name=None):
    return pl.pallas_call(
        body,
        out_shape=[jax.ShapeDtypeStruct(s, d) for s, d in outs],
        in_specs=[SMEM if smem_first and i == 0 else VMEM for i in range(n_in)],
        out_specs=[VMEM] * len(outs),
        scratch_shapes=list(scratch),
        cost_estimate=pl.CostEstimate(flops=flops, bytes_accessed=nbytes, transcendentals=0),
        compiler_params=pltpu.CompilerParams(vmem_limit_bytes=32 * 1024 * 1024),
        name=name,
    )


def silu(v):
    return v / (1.0 + jnp.exp(-v))


def first_kernel(latent, weight, bias, one, two, proj, act, row_up, row_dn, col_lf, col_rt, two_up, two_dn):
    rows, cols, _ = one.shape
    crows, ccols, _ = latent.shape
    for i in range(crows):
        p = jnp.dot(latent[i], weight[...], preferred_element_type=F32) + bias[...]
        p = p.astype(BF)
        proj[i] = p
        a = silu(p.astype(F32)).astype(BF)
        act[i] = a
        if i == 0:
            row_up[2 * cols :, :] = a
        if i == crows - 1:
            row_dn[2 * cols :, :] = a
        o = (rows + i) * B
        col_lf[o : o + B, :] = a[:B]
        col_rt[o : o + B, :] = a[ccols - B :]
    for k in range(2):
        row_up[k * cols : (k + 1) * cols, :] = one[k]
        row_dn[k * cols : (k + 1) * cols, :] = one[rows - 2 + k]
    two_up[...] = two[0]
    two_dn[...] = two[rows - 1]
    for i in range(rows):
        o, o2 = i * B, (rows + crows + i) * B
        col_lf[o : o + B, :] = one[i, :B]
        col_rt[o : o + B, :] = one[i, cols - B :]
        col_lf[o2 : o2 + B, :] = two[i, :B]
        col_rt[o2 : o2 + B, :] = two[i, cols - B :]


def corner_kernel(rows, crows, from_right, from_left, merged, up, dn):
    low = lax.broadcasted_iota(jnp.int32, (B, 128), 0) < B // 2

    def block(i):
        s = slice(i * B, (i + 1) * B)
        return jnp.where(low, from_right[s, :].astype(F32), from_left[s, :].astype(F32)).astype(BF)

    for i in range(2 * rows + crows):
        b = block(i)
        merged[i * B : (i + 1) * B, :] = b
        for dst, picks in ((up, (0, 1, rows, rows + crows)), (dn, (rows - 2, rows - 1, rows + crows - 1, 2 * rows + crows - 1))):
            if i in picks:
                k = picks.index(i)
                dst[k * B : (k + 1) * B, :] = b


def blocks_of(merged, above, below, first, count, corner_first, corners):
    get = lambda ref, i: ref[i * B : (i + 1) * B, :].astype(F32)
    return (
        [get(above, corner_first + k) for k in range(corners)]
        + [get(merged, first + i) for i in range(count)]
        + [get(below, corner_first + k) for k in range(corners)]
    )


def fill_frame(dst, interiors, blocks, cols):
    low = lax.broadcasted_iota(jnp.int32, (B, 128), 0) < B // 2
    zero = jnp.zeros((B, 128), F32)
    stride = cols + B
    n = len(interiors)
    dst[0:B, :] = jnp.where(low, zero, blocks[0]).astype(BF)
    for i in range(n):
        o = B + i * stride
        dst[o : o + cols, :] = interiors[i]()
        right = blocks[i]
        left = blocks[i + 1] if i + 1 < n else zero
        dst[o + cols : o + stride, :] = jnp.where(low, right, left).astype(BF)
    dst[B + n * stride :, :] = jnp.zeros((B, 128), BF)


def second_kernel(where_ref, one, act, merged, row_a, row_b, cor_a, cor_b, cache_frame, act_frame, send):
    rows, cols, _ = one.shape
    crows, ccols, _ = act.shape
    stride = cols + B
    blocks = blocks_of(merged, cor_a, cor_b, 0, rows, 0, 2)
    inter = (
        [functools.partial(lambda k: row_a[k * cols : (k + 1) * cols, :], k) for k in range(2)]
        + [functools.partial(lambda k: one[k], k) for k in range(rows)]
        + [functools.partial(lambda k: row_b[k * cols : (k + 1) * cols, :], k) for k in range(2)]
    )
    fill_frame(cache_frame, inter, blocks, cols)
    coarse = [row_a[2 * cols :, :]] + [act[i] for i in range(crows)] + [row_b[2 * cols :, :]]
    cblocks = blocks_of(merged, cor_a, cor_b, rows, crows, 2, 1)
    spread = (
        lax.broadcasted_iota(jnp.int32, (cols, ccols), 0) // 2 == lax.broadcasted_iota(jnp.int32, (cols, ccols), 1)
    ).astype(F32).astype(BF)
    low = lax.broadcasted_iota(jnp.int32, (B, 128), 0) < B // 2
    zero = jnp.zeros((1, 128), F32)
    last = [b[0:1] for b in cblocks], [b[B - 1 : B] for b in cblocks] + [zero]
    n = crows + 2
    act_frame[0:B, :] = jnp.where(low, 0.0, jnp.broadcast_to(last[1][0], (B, 128))).astype(BF)
    for m in range(0, n, 2):
        wide = jnp.dot(spread, jnp.concatenate([coarse[m], coarse[m + 1]], axis=1), preferred_element_type=F32).astype(BF)
        for h in range(2):
            for k in range(2):
                i = 2 * (m + h) + k
                o = B + i * stride
                act_frame[o : o + cols, :] = wide[:, h * 128 : (h + 1) * 128]
                right = jnp.broadcast_to(last[0][m + h], (B, 128))
                left = jnp.broadcast_to(last[1][m + h + k], (B, 128))
                act_frame[o + cols : o + stride, :] = jnp.where(low, right, left).astype(BF)
    act_frame[B + 2 * n * stride :, :] = jnp.zeros((B, 128), BF)
    leading = where_ref[0] == 0

    @pl.when(leading)
    def _():
        send[...] = act_frame[...]

    @pl.when(jnp.logical_not(leading))
    def _():
        send[...] = cache_frame[...]


def second_cache_kernel(two, merged, two_a, two_b, cor_a, cor_b, frame, *, first):
    rows, cols, _ = two.shape
    blocks = blocks_of(merged, cor_a, cor_b, first, rows, 3, 1)
    inter = [lambda: two_a[...]] + [functools.partial(lambda k: two[k], k) for k in range(rows)] + [lambda: two_b[...]]
    fill_frame(frame, inter, blocks, cols)


def taps_into(summed, frames, steps, weight, stride, chunk, k):
    lo = 0 if k == 0 else B + k * stride
    hi = B + (k + 1) * stride
    pieces, w01, w2 = [], [], []
    for ref, a in zip(frames, steps):
        for p in range(3):
            pieces.append(ref[lo + p * stride : hi + p * stride, :])
            w01.append(jnp.concatenate([weight[a, p, 0], weight[a, p, 1]], axis=1))
            w2.append(weight[a, p, 2])
    lhs = jnp.concatenate(pieces, axis=1)
    y01 = jnp.dot(lhs, jnp.concatenate(w01, axis=0), preferred_element_type=F32)
    y2 = jnp.dot(lhs, jnp.concatenate(w2, axis=0), preferred_element_type=F32)
    summed[8 + lo : 8 + hi, 0:256] = y01
    summed[8 + lo : 8 + hi, 256:384] = y2


def shifted(summed, lo, hi):
    return (
        summed[7 + lo : 7 + hi, 0:128] + summed[8 + lo : 8 + hi, 128:256] + summed[9 + lo : 9 + hi, 256:384]
    )


def conv_one_kernel(where_ref, cache, act, middle, weight, bias, two_frame, out, send, summed, *, cols, n_out):
    stride = cols + B
    frm, row, rows_n, col, cols_n = (where_ref[i] for i in range(5))
    t = lax.broadcasted_iota(jnp.int32, (B, 128), 0)
    keep_right = (col != cols_n - 1).astype(F32)
    keep_left = (col != 0).astype(F32)
    row_ok = [jnp.float32(1.0)] * n_out
    row_ok[0] = (row != 0).astype(F32)
    row_ok[-1] = (row != rows_n - 1).astype(F32)
    for k in range(n_out + 1):
        if k < n_out:
            taps_into(summed, (cache, middle, act), (0, 1, 2), weight, stride, None, k)
        lo = k * stride
        right = keep_right * row_ok[k - 1] if k > 0 else jnp.float32(0.0)
        left = keep_left * row_ok[k] if k < n_out else jnp.float32(0.0)
        keep = jnp.where(t == 0, right, jnp.where(t == B - 1, left, 0.0))
        v = shifted(summed, lo, lo + B) + bias[...]
        out[lo : lo + B, :] = jnp.where(keep > 0.0, silu(v), 0.0).astype(BF)
        if k < n_out:
            v = silu(shifted(summed, lo + B, lo + stride) + bias[...])
            if k in (0, n_out - 1):
                v = jnp.where(row_ok[k] > 0.0, v, 0.0)
            out[lo + B : lo + stride, :] = v.astype(BF)
    out[n_out * stride + B :, :] = jnp.zeros((B, 128), BF)

    @pl.when(frm == 0)
    def _():
        send[...] = out[...]

    @pl.when(frm != 0)
    def _():
        send[...] = two_frame[...]


def conv_two_kernel(cache, act, middle, weight, bias, proj, out, summed):
    n_out, cols, _ = out.shape
    ccols = proj.shape[1]
    stride = cols + B
    spread = (
        lax.broadcasted_iota(jnp.int32, (cols, ccols), 0) // 2 == lax.broadcasted_iota(jnp.int32, (cols, ccols), 1)
    ).astype(F32).astype(BF)
    for k in range(n_out):
        if k % 4 == 0:
            wide = jnp.dot(spread, jnp.concatenate([proj[k // 2], proj[k // 2 + 1]], axis=1), preferred_element_type=F32)
        taps_into(summed, (cache, middle, act), (0, 1, 2), weight, stride, None, k)
        lo = k * stride
        h = (k % 4) // 2
        v = shifted(summed, lo + B, lo + stride) + bias[...] + wide[:, h * 128 : (h + 1) * 128]
        out[k] = v.astype(BF)


def shift(x, axis, step):
    n = lax.axis_size(axis)
    return lax.ppermute(x, axis, [(i, i + step) for i in range(n) if 0 <= i + step < n])


def swap(x):
    return lax.ppermute(x, "frm", [(0, 1), (1, 0)])


def per_device(latent, proj_weight, proj_bias, cache_one, cache_two, conv_one, bias_one, conv_two, bias_two):
    latent, one, two = latent[0], cache_one[0], cache_two[0]
    rows, cols, ch = one.shape
    crows, ccols, _ = latent.shape
    stride = cols + B
    place = jnp.stack(
        [
            lax.axis_index("frm"),
            lax.axis_index("row"),
            jnp.int32(lax.axis_size("row")),
            lax.axis_index("col"),
            jnp.int32(lax.axis_size("col")),
        ]
    ).astype(jnp.int32)
    n_edge = (2 * rows + crows) * B
    proj, act, row_up, row_dn, col_lf, col_rt, two_up, two_dn = call(
        first_kernel,
        [
            ((crows, ccols, ch), BF),
            ((crows, ccols, ch), BF),
            ((2 * cols + ccols, ch), BF),
            ((2 * cols + ccols, ch), BF),
            ((n_edge, ch), BF),
            ((n_edge, ch), BF),
            ((cols, ch), BF),
            ((cols, ch), BF),
        ],
        n_in=5,
        flops=10**8,
        nbytes=2 * 10**6,
        name="first",
    )(latent, proj_weight, proj_bias.reshape(1, ch), one, two)
    from_right = shift(col_lf, "col", -1)
    from_left = shift(col_rt, "col", 1)
    row_b = shift(row_up, "row", -1)
    row_a = shift(row_dn, "row", 1)
    merged, cor_up, cor_dn = call(
        functools.partial(corner_kernel, rows, crows),
        [((n_edge, ch), BF), ((4 * B, ch), BF), ((4 * B, ch), BF)],
        n_in=2,
        flops=10**6,
        nbytes=2 * 10**5,
        name="corner",
    )(from_right, from_left)
    cor_b = shift(cor_up, "row", -1)
    cor_a = shift(cor_dn, "row", 1)
    two_b = shift(two_up, "row", -1)
    two_a = shift(two_dn, "row", 1)
    long_one = 2 * B + (rows + 4) * stride
    long_two = 2 * B + (rows + 2) * stride
    cache_frame, act_frame, send = call(
        second_kernel,
        [((long_one, ch), BF)] * 3,
        n_in=8,
        smem_first=True,
        flops=10**8,
        nbytes=4 * 10**6,
        name="frames",
    )(place, one, act, merged, row_a, row_b, cor_a, cor_b)
    middle = swap(send)
    (two_frame,) = call(
        functools.partial(second_cache_kernel, first=rows + crows),
        [((long_two, ch), BF)],
        n_in=6,
        flops=10**7,
        nbytes=2 * 10**6,
        name="frames_two",
    )(two, merged, two_a, two_b, cor_a, cor_b)
    conv_flops = 2 * 27 * ch * ch * rows * cols
    n_one = rows + 2
    act_two, send_two = call(
        functools.partial(conv_one_kernel, cols=cols, n_out=n_one),
        [((long_two, ch), BF)] * 2,
        scratch=[pltpu.VMEM((8 + B + n_one * stride + B + 8, 3 * ch), F32)],
        n_in=7,
        smem_first=True,
        flops=conv_flops,
        nbytes=6 * 10**6,
        name="conv_one",
    )(place, cache_frame, act_frame, middle, conv_one, bias_one.reshape(1, ch), two_frame)
    middle_two = swap(send_two)
    (decoded,) = call(
        conv_two_kernel,
        [((rows, cols, ch), BF)],
        scratch=[pltpu.VMEM((8 + B + rows * stride + 8, 3 * ch), F32)],
        n_in=6,
        flops=conv_flops,
        nbytes=6 * 10**6,
        name="conv_two",
    )(two_frame, act_two, middle_two, conv_two, bias_two.reshape(1, ch), proj)
    return decoded[None]


def solution(mesh):
    placed = (
        P(("grp", "frm"), "row", "col", None),
        P(),
        P(),
        P(("grp", "frm"), "row", "col", None),
        P(("grp", "frm"), "row", "col", None),
        P(),
        P(),
        P(),
        P(),
    )
    return jax.shard_map(
        per_device,
        mesh=mesh,
        in_specs=placed,
        out_specs=P(("grp", "frm"), "row", "col", None),
        check_vma=False,
    )
```

```python
import functools

import jax
import jax.numpy as jnp
from jax import lax
from jax.experimental import pallas as pl
from jax.experimental.pallas import tpu as pltpu
from jax.sharding import PartitionSpec as P

B = 16
BF = jnp.bfloat16
F32 = jnp.float32
VMEM = pl.BlockSpec(memory_space=pltpu.VMEM)
SMEM = pl.BlockSpec(memory_space=pltpu.SMEM)
HBM = pl.BlockSpec(memory_space=pltpu.HBM)


def call(body, outs, specs, scratch=(), flops=0, nbytes=0, limit=24):
    run = pl.pallas_call(
        body,
        out_shape=[jax.ShapeDtypeStruct(s, d) for s, d in outs],
        in_specs=specs,
        out_specs=[VMEM] * len(outs),
        scratch_shapes=list(scratch),
        cost_estimate=pl.CostEstimate(flops=flops, bytes_accessed=nbytes, transcendentals=0),
        compiler_params=pltpu.CompilerParams(vmem_limit_bytes=int(limit * 1024 * 1024)),
    )
    held = lambda v, spec: pltpu.with_memory_space_constraint(v, pltpu.HBM) if spec is HBM else v
    return lambda *args: run(*(held(v, spec) for v, spec in zip(args, specs, strict=True)))


def silu(v):
    return v / (1.0 + jnp.exp(-v))


def low_half():
    return lax.broadcasted_iota(jnp.int32, (B, 128), 0) < B // 2


def spread_matrix(cols, ccols):
    fine = lax.broadcasted_iota(jnp.int32, (cols, ccols), 0)
    return (fine // 2 == lax.broadcasted_iota(jnp.int32, (cols, ccols), 1)).astype(F32).astype(BF)


def first_kernel(
    latent, weight, bias, one, two, bias_one, bias_two,
    proj, act, row_up, row_dn, col_lf, col_rt, b_one, b_two,
    latent_v, weight_v, bias_v, sems,
):
    rows, cols, _ = one.shape
    crows, ccols, _ = latent.shape
    copies = [(latent, latent_v), (weight, weight_v), (bias, bias_v)]
    n_first = len(copies)
    n_c1 = rows * B
    n_c2 = (rows + crows) * B
    for i in range(rows):
        copies.append((one.at[i, 0:B], col_lf.at[i * B : (i + 1) * B]))
        copies.append((one.at[i, cols - B : cols], col_rt.at[i * B : (i + 1) * B]))
        copies.append((two.at[i, 0:B], col_lf.at[n_c2 + i * B : n_c2 + (i + 1) * B]))
        copies.append((two.at[i, cols - B : cols], col_rt.at[n_c2 + i * B : n_c2 + (i + 1) * B]))
    t0 = 2 * cols + ccols
    for k in range(2):
        copies.append((one.at[k], row_up.at[k * cols : (k + 1) * cols]))
        copies.append((one.at[rows - 2 + k], row_dn.at[k * cols : (k + 1) * cols]))
    copies.append((two.at[0], row_up.at[t0 : t0 + cols]))
    copies.append((two.at[rows - 1], row_dn.at[t0 : t0 + cols]))
    copies.append((bias_one, b_one))
    copies.append((bias_two, b_two))
    started = [pltpu.make_async_copy(s, d, sems.at[i]) for i, (s, d) in enumerate(copies)]
    for c in started:
        c.start()
    for c in started[:n_first]:
        c.wait()
    for i in range(crows):
        p = (jnp.dot(latent_v[i], weight_v[...], preferred_element_type=F32) + bias_v[...]).astype(BF)
        proj[i] = p
        a = silu(p.astype(F32)).astype(BF)
        act[i] = a
        if i == 0:
            row_up[2 * cols : t0, :] = a
        if i == crows - 1:
            row_dn[2 * cols : t0, :] = a
        o = n_c1 + i * B
        col_lf[o : o + B, :] = a[:B]
        col_rt[o : o + B, :] = a[ccols - B :]
    for c in started[n_first:]:
        c.wait()


def corner_kernel(rows, crows, from_right, from_left, merged, up, dn):
    low = low_half()
    picks_up = (0, 1, rows, rows + crows)
    picks_dn = (rows - 2, rows - 1, rows + crows - 1, 2 * rows + crows - 1)
    for i in range(2 * rows + crows):
        s = slice(i * B, (i + 1) * B)
        b = jnp.where(low, from_right[s, :].astype(F32), from_left[s, :].astype(F32)).astype(BF)
        merged[s, :] = b
        for dst, picks in ((up, picks_up), (dn, picks_dn)):
            if i in picks:
                k = picks.index(i)
                dst[k * B : (k + 1) * B, :] = b


def block(ref, i):
    return ref[i * B : (i + 1) * B, :].astype(F32)


def spread_edge(m):
    return jnp.where(
        low_half(), jnp.broadcast_to(m[0:1], (B, 128)), jnp.broadcast_to(m[B - 1 : B], (B, 128))
    ).astype(BF)


def put_row(dst, i, inside, edges):
    cols = dst.shape[1] - 2 * B
    dst[i, 0:B, :] = edges
    dst[i, B : B + cols, :] = inside
    dst[i, B + cols :, :] = edges


def conv_rows(frames, steps, weight, k, sums, slot):
    span = sums.shape[1] - 16
    w01, w2 = [], []
    zero = jnp.zeros(weight.shape[3:], BF)
    for a in steps:
        for p in range(4):
            if p < 3:
                w01.append(jnp.concatenate([weight[a, p, 0], weight[a, p, 1]], axis=1))
            w2.append(jnp.concatenate([weight[a, p, 2] if p < 3 else zero, weight[a, p - 1, 2] if p else zero], axis=1))
    w01, w2 = jnp.concatenate(w01, axis=0), jnp.concatenate(w2, axis=0)
    lhs = jnp.concatenate([f(k + p) for f in frames for p in range(4)], axis=1)
    y2 = jnp.dot(lhs, w2, preferred_element_type=F32)
    results = []
    for h in range(2):
        lhs = jnp.concatenate([f(k + h + p) for f in frames for p in range(3)], axis=1)
        y01 = jnp.dot(lhs, w01, preferred_element_type=F32)
        s = 2 * slot + h
        sums[s, 8 : 8 + span, 0:128] = y01[:, 0:128]
        sums[s, 8 : 8 + span, 128:256] = y2[:, h * 128 : (h + 1) * 128]
        results.append(sums[s, 7 : 7 + span, 0:128] + y01[:, 128:256] + sums[s, 9 : 9 + span, 128:256])
    return results


def joined(core, border):
    n = core.shape[0]
    return lambda i: border[i] if i < 2 else core[i - 2] if i < n + 2 else border[i - n]


def inner_kernel(one, act, merged, weight, cache_core, act_core, part, sums):
    rows, cols, _ = one.shape
    crows, ccols, _ = act.shape
    for i in range(rows):
        put_row(cache_core, i, one[i], merged[i * B : (i + 1) * B, :])
    spread = spread_matrix(cols, ccols)
    for m in range(0, crows, 2):
        wide = jnp.dot(spread, jnp.concatenate([act[m], act[m + 1]], axis=1), preferred_element_type=F32).astype(BF)
        for h in range(2):
            edges = spread_edge(block(merged, rows + m + h))
            for i in range(2):
                put_row(act_core, 2 * (m + h) + i, wide[:, h * 128 : (h + 1) * 128], edges)
    frames = (lambda i: cache_core[i - 2], lambda i: act_core[i - 2])
    for n, k in enumerate(range(2, rows, 2)):
        for h, v in enumerate(conv_rows(frames, (0, 2), weight, k, sums, n % 2)):
            part[k - 2 + h] = v


def border_kernel(where_ref, row_a, row_b, cor_a, cor_b, cache_core, act_core, cache_border, act_border, send):
    rows, span, _ = cache_core.shape
    cols = span - 2 * B
    ccols = row_a.shape[0] - 3 * cols
    coarse = jnp.concatenate([row_a[2 * cols : 2 * cols + ccols, :], row_b[2 * cols : 2 * cols + ccols, :]], axis=1)
    wide = jnp.dot(spread_matrix(cols, ccols), coarse, preferred_element_type=F32).astype(BF)
    for h, (row, cor) in enumerate(((row_a, cor_a), (row_b, cor_b))):
        edges = spread_edge(block(cor, 2))
        for k in range(2):
            put_row(cache_border, 2 * h + k, row[k * cols : (k + 1) * cols, :], cor[k * B : (k + 1) * B, :])
            put_row(act_border, 2 * h + k, wide[:, h * 128 : (h + 1) * 128], edges)
    for lead, core, border in ((True, act_core, act_border), (False, cache_core, cache_border)):

        @pl.when((where_ref[0] == 0) == lead)
        def _(core=core, border=border):
            send[0:2] = border[0:2]
            send[2 : rows + 2] = core[...]
            send[rows + 2 :] = border[2:4]


def outer_kernel(cache_core, act_core, cache_border, act_border, weight, two, merged, row_a, row_b, cor_a, cor_b, part, two_frame, sums, *, first):
    rows, cols, _ = two.shape
    frames = (joined(cache_core, cache_border), joined(act_core, act_border))
    for n, k in enumerate((0, rows)):
        for h, v in enumerate(conv_rows(frames, (0, 2), weight, k, sums, n)):
            part[2 * n + h] = v
    t0 = row_a.shape[0] - cols
    put_row(two_frame, 0, row_a[t0:, :], cor_a[3 * B :, :])
    for i in range(rows):
        put_row(two_frame, i + 1, two[i], merged[(first + i) * B : (first + i + 1) * B, :])
    put_row(two_frame, rows + 1, row_b[t0:, :], cor_b[3 * B :, :])


def middle_kernel(where_ref, middle, part_in, part_out, weight, bias, two_frame, out, send, sums):
    n_out, span, _ = out.shape
    frm, row, rows_n, col, cols_n = (where_ref[i] for i in range(5))
    t = lax.broadcasted_iota(jnp.int32, (B, 128), 0)
    keep_left = (t != B - 1) | (col != 0)
    keep_right = (t != 0) | (col != cols_n - 1)
    part = joined(part_in, part_out)
    for k in range(0, n_out, 2):
        for h, v in enumerate(conv_rows((lambda i: middle[i],), (1,), weight, k, sums, k // 2 % 2)):
            i = k + h
            v = silu(v + part(i) + bias[...])
            if i == 0:
                v = jnp.where(row != 0, v, 0.0)
            if i == n_out - 1:
                v = jnp.where(row != rows_n - 1, v, 0.0)
            out[i, 0:B, :] = jnp.where(keep_left, v[0:B], 0.0).astype(BF)
            out[i, B : span - B, :] = v[B : span - B].astype(BF)
            out[i, span - B :, :] = jnp.where(keep_right, v[span - B :], 0.0).astype(BF)

    @pl.when(frm == 0)
    def _():
        send[...] = out[...]

    @pl.when(frm != 0)
    def _():
        send[...] = two_frame[...]


def own_two_kernel(two_frame, act_two, weight, proj, bias, part, sums):
    n_out, cols, _ = part.shape
    spread = spread_matrix(cols, proj.shape[1])
    frames = (lambda i: two_frame[i], lambda i: act_two[i])
    for k in range(0, n_out, 2):
        if k % 4 == 0:
            wide = jnp.dot(spread, jnp.concatenate([proj[k // 2], proj[k // 2 + 1]], axis=1), preferred_element_type=F32)
        base = wide[:, k % 4 * 64 : k % 4 * 64 + 128] + bias[...]
        for h, v in enumerate(conv_rows(frames, (0, 2), weight, k, sums, k // 2 % 2)):
            part[k + h] = v[B : B + cols] + base


def middle_two_kernel(middle, part, weight, out, sums):
    n_out, cols, _ = out.shape
    for k in range(0, n_out, 2):
        for h, v in enumerate(conv_rows((lambda i: middle[i],), (1,), weight, k, sums, k // 2 % 2)):
            out[k + h] = (part[k + h] + v[B : B + cols]).astype(BF)


def shift(x, axis, step):
    n = lax.axis_size(axis)
    return lax.ppermute(x, axis, [(i, i + step) for i in range(n) if 0 <= i + step < n])


def swap(x):
    return lax.ppermute(x, "frm", [(0, 1), (1, 0)])


def program(latent, proj_weight, proj_bias, cache_one, cache_two, conv_one, bias_one, conv_two, bias_two):
    latent, one, two = latent[0], cache_one[0], cache_two[0]
    rows, cols, ch = one.shape
    crows, ccols, lch = latent.shape
    span = cols + 2 * B
    place = jnp.stack(
        [
            lax.axis_index("frm"),
            lax.axis_index("row"),
            jnp.int32(lax.axis_size("row")),
            lax.axis_index("col"),
            jnp.int32(lax.axis_size("col")),
        ]
    ).astype(jnp.int32)
    n_edge = (2 * rows + crows) * B
    n_row = 3 * cols + ccols
    sums = pltpu.VMEM((4, span + 16, 2 * ch), F32)
    proj, act, row_up, row_dn, col_lf, col_rt, b_one, b_two = call(
        first_kernel,
        [
            ((crows, ccols, ch), BF),
            ((crows, ccols, ch), BF),
            ((n_row, ch), BF),
            ((n_row, ch), BF),
            ((n_edge, ch), BF),
            ((n_edge, ch), BF),
            ((1, ch), F32),
            ((1, ch), F32),
        ],
        [HBM] * 7,
        scratch=[
            pltpu.VMEM((crows, ccols, lch), BF),
            pltpu.VMEM((lch, ch), BF),
            pltpu.VMEM((1, ch), F32),
            pltpu.SemaphoreType.DMA((3 + 4 * rows + 8,)),
        ],
        flops=10**8,
        nbytes=2 * 10**6,
        limit=24,
    )(latent, proj_weight, proj_bias.reshape(1, ch), one, two, bias_one.reshape(1, ch), bias_two.reshape(1, ch))
    from_left = shift(col_rt, "col", 1)
    from_right = shift(col_lf, "col", -1)
    row_a = shift(row_dn, "row", 1)
    row_b = shift(row_up, "row", -1)
    merged, cor_up, cor_dn = call(
        functools.partial(corner_kernel, rows, crows),
        [((n_edge, ch), BF), ((4 * B, ch), BF), ((4 * B, ch), BF)],
        [VMEM] * 2,
        flops=10**6,
        nbytes=2 * 10**5,
    )(from_right, from_left)
    cor_a = shift(cor_dn, "row", 1)
    cor_b = shift(cor_up, "row", -1)
    third = 2 * 9 * ch * ch * rows * cols
    cache_core, act_core, part_in = call(
        inner_kernel,
        [((rows, span, ch), BF), ((rows, span, ch), BF), ((rows - 2, span, ch), F32)],
        [VMEM] * 4,
        scratch=[sums],
        flops=2 * third,
        nbytes=4 * 10**6,
    )(one, act, merged, conv_one)
    cache_border, act_border, send = call(
        border_kernel,
        [((4, span, ch), BF), ((4, span, ch), BF), ((rows + 4, span, ch), BF)],
        [SMEM] + [VMEM] * 6,
        flops=10**8,
        nbytes=4 * 10**6,
    )(place, row_a, row_b, cor_a, cor_b, cache_core, act_core)
    middle = swap(send)
    part_out, two_frame = call(
        functools.partial(outer_kernel, first=rows + crows),
        [((4, span, ch), F32), ((rows + 2, span, ch), BF)],
        [VMEM] * 11,
        scratch=[sums],
        flops=third,
        nbytes=4 * 10**6,
    )(cache_core, act_core, cache_border, act_border, conv_one, two, merged, row_a, row_b, cor_a, cor_b)
    act_two, send_two = call(
        middle_kernel,
        [((rows + 2, span, ch), BF)] * 2,
        [SMEM] + [VMEM] * 6,
        scratch=[sums],
        flops=third,
        nbytes=6 * 10**6,
    )(place, middle, part_in, part_out, conv_one, b_one, two_frame)
    middle_two = swap(send_two)
    (part_two,) = call(
        own_two_kernel, [((rows, cols, ch), F32)], [VMEM] * 5, scratch=[sums], flops=2 * third, nbytes=6 * 10**6
    )(two_frame, act_two, conv_two, proj, b_two)
    (decoded,) = call(
        middle_two_kernel, [((rows, cols, ch), BF)], [VMEM] * 3, scratch=[sums], flops=third, nbytes=6 * 10**6
    )(middle_two, part_two, conv_two)
    return decoded[None]


def solution(mesh):
    placed = (
        P(("grp", "frm"), "row", "col", None),
        P(),
        P(),
        P(("grp", "frm"), "row", "col", None),
        P(("grp", "frm"), "row", "col", None),
        P(),
        P(),
        P(),
        P(),
    )
    return jax.shard_map(
        program,
        mesh=mesh,
        in_specs=placed,
        out_specs=P(("grp", "frm"), "row", "col", None),
        check_vma=False,
    )
```

```python
import functools

import jax
import jax.numpy as jnp
from jax import lax
from jax.experimental import pallas as pl
from jax.experimental.pallas import tpu as pltpu
from jax.sharding import PartitionSpec as P

B = 16
BF = jnp.bfloat16
F32 = jnp.float32
VMEM = pl.BlockSpec(memory_space=pltpu.VMEM)
HBM = pl.BlockSpec(memory_space=pltpu.HBM)


def call(body, outs, specs, scratch=(), flops=0, nbytes=0, limit=24):
    run = pl.pallas_call(
        body,
        out_shape=[jax.ShapeDtypeStruct(s, d) for s, d in outs],
        in_specs=specs,
        out_specs=[VMEM] * len(outs),
        scratch_shapes=list(scratch),
        cost_estimate=pl.CostEstimate(flops=flops, bytes_accessed=nbytes, transcendentals=0),
        compiler_params=pltpu.CompilerParams(vmem_limit_bytes=int(limit * 1024 * 1024)),
    )
    held = lambda v, spec: pltpu.with_memory_space_constraint(v, pltpu.HBM) if spec is HBM else v
    return lambda *args: run(*(held(v, spec) for v, spec in zip(args, specs, strict=True)))


def silu(v):
    return v / (1.0 + jnp.exp(-v))


def low_half():
    return lax.broadcasted_iota(jnp.int32, (B, 128), 0) < B // 2


def spread_matrix(cols, ccols):
    fine = lax.broadcasted_iota(jnp.int32, (cols, ccols), 0)
    return (fine // 2 == lax.broadcasted_iota(jnp.int32, (cols, ccols), 1)).astype(F32).astype(BF)


def even(axis):
    return lax.rem(lax.axis_index(axis), 2) == 0


def pick(axis, high, low, step=1):
    start = jnp.where(even(axis), high, low)
    return pl.multiple_of(start, step) if step > 1 else start


def first_kernel(
    latent, weight, bias, one, two, bias_one, bias_two,
    proj, act, row_0, row_1, col_0, col_1, b_one, b_two,
    latent_v, weight_v, bias_v, sems,
):
    rows, cols, _ = one.shape
    crows, ccols, _ = latent.shape
    copies = [(latent, latent_v), (weight, weight_v), (bias, bias_v)]
    n_first = len(copies)
    n_c1 = rows * B
    n_c2 = (rows + crows) * B
    t0 = 2 * cols + ccols
    sends = ((row_0, col_0, False), (row_1, col_1, True))
    for row_s, col_s, flip in sends:
        lo, hi = (cols - B, 0) if flip else (0, cols - B)
        c = pl.ds(pick("col", hi, lo, B), B)
        for i in range(rows):
            copies.append((one.at[i, c], col_s.at[i * B : (i + 1) * B]))
            copies.append((two.at[i, c], col_s.at[n_c2 + i * B : n_c2 + (i + 1) * B]))
        lo, hi = (rows - 2, 0) if flip else (0, rows - 2)
        r = pick("row", hi, lo)
        for k in range(2):
            copies.append((one.at[r + k], row_s.at[k * cols : (k + 1) * cols]))
        lo, hi = (rows - 1, 0) if flip else (0, rows - 1)
        copies.append((two.at[pick("row", hi, lo)], row_s.at[t0 : t0 + cols]))
    copies.append((bias_one, b_one))
    copies.append((bias_two, b_two))
    started = [pltpu.make_async_copy(s, d, sems.at[i]) for i, (s, d) in enumerate(copies)]
    for c in started:
        c.start()
    for c in started[:n_first]:
        c.wait()
    for i in range(crows):
        p = (jnp.dot(latent_v[i], weight_v[...], preferred_element_type=F32) + bias_v[...]).astype(BF)
        proj[i] = p
        act[i] = silu(p.astype(F32)).astype(BF)
    for row_s, col_s, flip in sends:
        lo, hi = (crows - 1, 0) if flip else (0, crows - 1)
        row_s[2 * cols : t0, :] = act[pick("row", hi, lo)]
        lo, hi = (ccols - B, 0) if flip else (0, ccols - B)
        c = pl.ds(pick("col", hi, lo, B), B)
        for i in range(crows):
            col_s[n_c1 + i * B : n_c1 + (i + 1) * B, :] = act[i, c, :]
    for c in started[n_first:]:
        c.wait()


def corner_kernel(rows, crows, got_0, got_1, merged, cor_0, cor_1):
    take_0 = low_half() == even("col")
    for i in range(2 * rows + crows):
        s = slice(i * B, (i + 1) * B)
        merged[s, :] = jnp.where(take_0, got_0[s, :].astype(F32), got_1[s, :].astype(F32)).astype(BF)
    lows = (0, 1, rows, rows + crows)
    highs = (rows - 2, rows - 1, rows + crows - 1, 2 * rows + crows - 1)
    for k, (lo, hi) in enumerate(zip(lows, highs)):
        s = slice(k * B, (k + 1) * B)
        cor_0[s, :] = merged[pl.ds(pick("row", hi * B, lo * B, B), B), :]
        cor_1[s, :] = merged[pl.ds(pick("row", lo * B, hi * B, B), B), :]


def block(ref, i):
    return ref[i * B : (i + 1) * B, :].astype(F32)


def spread_edge(m):
    return jnp.where(
        low_half(), jnp.broadcast_to(m[0:1], (B, 128)), jnp.broadcast_to(m[B - 1 : B], (B, 128))
    ).astype(BF)


def put_row(dst, i, inside, edges):
    cols = dst.shape[1] - 2 * B
    dst[i, 0:B, :] = edges
    dst[i, B : B + cols, :] = inside
    dst[i, B + cols :, :] = edges


def conv_rows(frames, steps, weight, k, sums, slot):
    span = sums.shape[1] - 16
    w01, w2 = [], []
    zero = jnp.zeros(weight.shape[3:], BF)
    for a in steps:
        for p in range(4):
            if p < 3:
                w01.append(jnp.concatenate([weight[a, p, 0], weight[a, p, 1]], axis=1))
            w2.append(jnp.concatenate([weight[a, p, 2] if p < 3 else zero, weight[a, p - 1, 2] if p else zero], axis=1))
    w01, w2 = jnp.concatenate(w01, axis=0), jnp.concatenate(w2, axis=0)
    lhs = jnp.concatenate([f(k + p) for f in frames for p in range(4)], axis=1)
    y2 = jnp.dot(lhs, w2, preferred_element_type=F32)
    results = []
    for h in range(2):
        lhs = jnp.concatenate([f(k + h + p) for f in frames for p in range(3)], axis=1)
        y01 = jnp.dot(lhs, w01, preferred_element_type=F32)
        s = 2 * slot + h
        sums[s, 8 : 8 + span, 0:128] = y01[:, 0:128]
        sums[s, 8 : 8 + span, 128:256] = y2[:, h * 128 : (h + 1) * 128]
        results.append(sums[s, 7 : 7 + span, 0:128] + y01[:, 128:256] + sums[s, 9 : 9 + span, 128:256])
    return results


def joined(core, border):
    n = core.shape[0]
    return lambda i: border[i] if i < 2 else core[i - 2] if i < n + 2 else border[i - n]


def fill_kernel(one, act, merged, cache_core, act_core, send):
    rows, cols, _ = one.shape
    crows, ccols, _ = act.shape
    for i in range(rows):
        put_row(cache_core, i, one[i], merged[i * B : (i + 1) * B, :])
    spread = spread_matrix(cols, ccols)
    for m in range(0, crows, 2):
        wide = jnp.dot(spread, jnp.concatenate([act[m], act[m + 1]], axis=1), preferred_element_type=F32).astype(BF)
        for h in range(2):
            edges = spread_edge(block(merged, rows + m + h))
            for i in range(2):
                put_row(act_core, 2 * (m + h) + i, wide[:, h * 128 : (h + 1) * 128], edges)
    choose(send, act_core, cache_core)


def choose(send, leading, other):
    for first, src in ((True, leading), (False, other)):

        @pl.when((lax.axis_index("frm") == 0) == first)
        def _(src=src):
            send[...] = src[...]


def inner_kernel(cache_core, act_core, weight, part, sums):
    frames = (lambda i: cache_core[i - 2], lambda i: act_core[i - 2])
    for n, k in enumerate(range(2, 2 + part.shape[0], 2)):
        for h, v in enumerate(conv_rows(frames, (0, 2), weight, k, sums, n % 2)):
            part[k - 2 + h] = v


def border_kernel(row_0, row_1, cor_0, cor_1, cache_border, act_border, send):
    _, span, _ = cache_border.shape
    cols = span - 2 * B
    ccols = row_0.shape[0] - 3 * cols
    for lead in (True, False):

        @pl.when(even("row") == lead)
        def _(lead=lead):
            pairs = ((row_1, cor_1), (row_0, cor_0)) if lead else ((row_0, cor_0), (row_1, cor_1))
            coarse = jnp.concatenate([row[2 * cols : 2 * cols + ccols, :] for row, _ in pairs], axis=1)
            wide = jnp.dot(spread_matrix(cols, ccols), coarse, preferred_element_type=F32).astype(BF)
            for h, (row, cor) in enumerate(pairs):
                edges = spread_edge(block(cor, 2))
                for k in range(2):
                    put_row(cache_border, 2 * h + k, row[k * cols : (k + 1) * cols, :], cor[k * B : (k + 1) * B, :])
                    put_row(act_border, 2 * h + k, wide[:, h * 128 : (h + 1) * 128], edges)

    choose(send, act_border, cache_border)


def outer_kernel(cache_core, act_core, cache_border, act_border, weight, two, merged, row_0, row_1, cor_0, cor_1, part, two_frame, sums, *, first):
    rows, cols, _ = two.shape
    frames = (joined(cache_core, cache_border), joined(act_core, act_border))
    for n, k in enumerate((0, rows)):
        for h, v in enumerate(conv_rows(frames, (0, 2), weight, k, sums, n)):
            part[2 * n + h] = v
    t0 = row_0.shape[0] - cols
    for i in range(rows):
        put_row(two_frame, i + 1, two[i], merged[(first + i) * B : (first + i + 1) * B, :])
    for lead in (True, False):

        @pl.when(even("row") == lead)
        def _(lead=lead):
            put_row(two_frame, rows + 1 if lead else 0, row_0[t0:, :], cor_0[3 * B :, :])
            put_row(two_frame, 0 if lead else rows + 1, row_1[t0:, :], cor_1[3 * B :, :])


def finish_row(out, i, v, row, n_out):
    span = v.shape[0]
    t = lax.broadcasted_iota(jnp.int32, (B, 128), 0)
    keep_left = (t != B - 1) | (lax.axis_index("col") != 0)
    keep_right = (t != 0) | (lax.axis_index("col") != lax.axis_size("col") - 1)
    v = silu(v)
    if row == 0:
        v = jnp.where(lax.axis_index("row") != 0, v, 0.0)
    if row == n_out - 1:
        v = jnp.where(lax.axis_index("row") != lax.axis_size("row") - 1, v, 0.0)
    out[i, 0:B, :] = jnp.where(keep_left, v[0:B], 0.0).astype(BF)
    out[i, B : span - B, :] = v[B : span - B].astype(BF)
    out[i, span - B :, :] = jnp.where(keep_right, v[span - B :], 0.0).astype(BF)


def middle_inner_kernel(core, part, weight, bias, out, sums):
    n = out.shape[0]
    for m in range(0, n, 2):
        for h, v in enumerate(conv_rows((lambda i: core[i - 2],), (1,), weight, m + 2, sums, m // 2 % 2)):
            finish_row(out, m + h, v + part[m + h] + bias[...], m + h + 2, n + 4)


def middle_outer_kernel(core, border, part, weight, bias, inner, two_frame, out, send, sums):
    n_out = out.shape[0]
    frame = joined(core, border)
    for n, k in enumerate((0, n_out - 2)):
        for h, v in enumerate(conv_rows((frame,), (1,), weight, k, sums, n)):
            finish_row(out, k + h, v + part[2 * n + h] + bias[...], k + h, n_out)
    out[2 : n_out - 2] = inner[...]
    choose(send, out, two_frame)


def own_two_kernel(two_frame, act_two, weight, proj, bias, part, sums):
    n_out, cols, _ = part.shape
    spread = spread_matrix(cols, proj.shape[1])
    frames = (lambda i: two_frame[i], lambda i: act_two[i])
    for k in range(0, n_out, 2):
        if k % 4 == 0:
            wide = jnp.dot(spread, jnp.concatenate([proj[k // 2], proj[k // 2 + 1]], axis=1), preferred_element_type=F32)
        base = wide[:, k % 4 * 64 : k % 4 * 64 + 128] + bias[...]
        for h, v in enumerate(conv_rows(frames, (0, 2), weight, k, sums, k // 2 % 2)):
            part[k + h] = v[B : B + cols] + base


def middle_two_kernel(middle, part, weight, out, sums):
    n_out, cols, _ = out.shape
    for k in range(0, n_out, 2):
        for h, v in enumerate(conv_rows((lambda i: middle[i],), (1,), weight, k, sums, k // 2 % 2)):
            out[k + h] = (part[k + h] + v[B : B + cols]).astype(BF)


def exchange(x, axis, first):
    pairs = [(i, i + 1) for i in range(first, lax.axis_size(axis) - 1, 2)]
    return lax.ppermute(x, axis, pairs + [(j, i) for i, j in pairs])


def swap(x):
    return lax.ppermute(x, "frm", [(0, 1), (1, 0)])


def program(latent, proj_weight, proj_bias, cache_one, cache_two, conv_one, bias_one, conv_two, bias_two):
    latent, one, two = latent[0], cache_one[0], cache_two[0]
    rows, cols, ch = one.shape
    crows, ccols, lch = latent.shape
    span = cols + 2 * B
    n_edge = (2 * rows + crows) * B
    n_row = 3 * cols + ccols
    sums = pltpu.VMEM((4, span + 16, 2 * ch), F32)
    proj, act, row_0, row_1, col_0, col_1, b_one, b_two = call(
        first_kernel,
        [
            ((crows, ccols, ch), BF),
            ((crows, ccols, ch), BF),
            ((n_row, ch), BF),
            ((n_row, ch), BF),
            ((n_edge, ch), BF),
            ((n_edge, ch), BF),
            ((1, ch), F32),
            ((1, ch), F32),
        ],
        [HBM] * 7,
        scratch=[
            pltpu.VMEM((crows, ccols, lch), BF),
            pltpu.VMEM((lch, ch), BF),
            pltpu.VMEM((1, ch), F32),
            pltpu.SemaphoreType.DMA((3 + 4 * rows + 8,)),
        ],
        flops=10**8,
        nbytes=2 * 10**6,
        limit=24,
    )(latent, proj_weight, proj_bias.reshape(1, ch), one, two, bias_one.reshape(1, ch), bias_two.reshape(1, ch))
    got_1 = exchange(col_1, "col", 1)
    got_0 = exchange(col_0, "col", 0)
    row_1 = exchange(row_1, "row", 1)
    row_0 = exchange(row_0, "row", 0)
    merged, cor_0, cor_1 = call(
        functools.partial(corner_kernel, rows, crows),
        [((n_edge, ch), BF), ((4 * B, ch), BF), ((4 * B, ch), BF)],
        [VMEM] * 2,
        flops=10**6,
        nbytes=2 * 10**5,
    )(got_0, got_1)
    cor_1 = exchange(cor_1, "row", 1)
    cor_0 = exchange(cor_0, "row", 0)
    third = 2 * 9 * ch * ch * rows * cols
    core_shape, border_shape = ((rows, span, ch), BF), ((4, span, ch), BF)
    cache_core, act_core, send_core = call(
        fill_kernel, [core_shape] * 3, [VMEM] * 3, flops=10**8, nbytes=4 * 10**6
    )(one, act, merged)
    middle_core = swap(send_core)
    (part_in,) = call(
        inner_kernel, [((rows - 2, span, ch), F32)], [VMEM] * 3, scratch=[sums], flops=2 * third, nbytes=4 * 10**6
    )(cache_core, act_core, conv_one)
    cache_border, act_border, send_border = call(
        border_kernel, [border_shape] * 3, [VMEM] * 4, flops=10**8, nbytes=4 * 10**6
    )(row_0, row_1, cor_0, cor_1)
    middle_border = swap(send_border)
    part_out, two_frame = call(
        functools.partial(outer_kernel, first=rows + crows),
        [((4, span, ch), F32), ((rows + 2, span, ch), BF)],
        [VMEM] * 11,
        scratch=[sums],
        flops=third,
        nbytes=4 * 10**6,
    )(cache_core, act_core, cache_border, act_border, conv_one, two, merged, row_0, row_1, cor_0, cor_1)
    (act_inner,) = call(
        middle_inner_kernel, [((rows - 2, span, ch), BF)], [VMEM] * 4, scratch=[sums], flops=third, nbytes=6 * 10**6
    )(middle_core, part_in, conv_one, b_one)
    act_two, send_two = call(
        middle_outer_kernel,
        [((rows + 2, span, ch), BF)] * 2,
        [VMEM] * 7,
        scratch=[sums],
        flops=third // 2,
        nbytes=6 * 10**6,
    )(middle_core, middle_border, part_out, conv_one, b_one, act_inner, two_frame)
    middle_two = swap(send_two)
    (part_two,) = call(
        own_two_kernel, [((rows, cols, ch), F32)], [VMEM] * 5, scratch=[sums], flops=2 * third, nbytes=6 * 10**6
    )(two_frame, act_two, conv_two, proj, b_two)
    (decoded,) = call(
        middle_two_kernel, [((rows, cols, ch), BF)], [VMEM] * 3, scratch=[sums], flops=third, nbytes=6 * 10**6
    )(middle_two, part_two, conv_two)
    return decoded[None]


def solution(mesh):
    placed = (
        P(("grp", "frm"), "row", "col", None),
        P(),
        P(),
        P(("grp", "frm"), "row", "col", None),
        P(("grp", "frm"), "row", "col", None),
        P(),
        P(),
        P(),
        P(),
    )
    return jax.shard_map(
        program,
        mesh=mesh,
        in_specs=placed,
        out_specs=P(("grp", "frm"), "row", "col", None),
        check_vma=False,
    )
```

```python
import functools

import jax
import jax.numpy as jnp
from jax import lax
from jax.experimental import pallas as pl
from jax.experimental.pallas import tpu as pltpu
from jax.sharding import PartitionSpec as P

B = 16
E = B // 2
BF = jnp.bfloat16
F32 = jnp.float32
VMEM = pl.BlockSpec(memory_space=pltpu.VMEM)
HBM = pl.BlockSpec(memory_space=pltpu.HBM)


def call(body, outs, specs, scratch=(), flops=0, nbytes=0, limit=24, out_specs=None):
    run = pl.pallas_call(
        body,
        out_shape=[jax.ShapeDtypeStruct(s, d) for s, d in outs],
        in_specs=specs,
        out_specs=out_specs or [VMEM] * len(outs),
        scratch_shapes=list(scratch),
        cost_estimate=pl.CostEstimate(flops=flops, bytes_accessed=nbytes, transcendentals=0),
        compiler_params=pltpu.CompilerParams(vmem_limit_bytes=int(limit * 1024 * 1024)),
    )
    held = lambda v, spec: pltpu.with_memory_space_constraint(v, pltpu.HBM) if spec is HBM else v
    return lambda *args: run(*(held(v, spec) for v, spec in zip(args, specs, strict=True)))


def silu(v):
    return v / (1.0 + jnp.exp(-v))


def low_half():
    return lax.broadcasted_iota(jnp.int32, (B, 128), 0) < B // 2


def spread_matrix(cols, ccols):
    fine = lax.broadcasted_iota(jnp.int32, (cols, ccols), 0)
    return (fine // 2 == lax.broadcasted_iota(jnp.int32, (cols, ccols), 1)).astype(F32).astype(BF)


def even(axis):
    return lax.rem(lax.axis_index(axis), 2) == 0


def pick(axis, high, low, step=1):
    start = jnp.where(even(axis), high, low)
    return pl.multiple_of(start, step) if step > 1 else start


def first_kernel(
    latent, weight, bias, one, two, bias_one, bias_two,
    proj, act, row_0, row_1, col_0, col_1, b_one, b_two,
    latent_v, weight_v, bias_v, sems,
):
    rows, cols, _ = one.shape
    crows, ccols, _ = latent.shape
    copies = [(latent, latent_v), (weight, weight_v), (bias, bias_v)]
    n_first = len(copies)
    n_c1 = rows * E
    n_c2 = (rows + crows) * E
    t0 = 2 * cols + ccols
    sends = ((row_0, col_0, False), (row_1, col_1, True))
    for row_s, col_s, flip in sends:
        lo, hi = (cols - E, 0) if flip else (0, cols - E)
        c = pl.ds(pick("col", hi, lo, E), E)
        for i in range(rows):
            copies.append((one.at[i, c], col_s.at[i * E : (i + 1) * E]))
            copies.append((two.at[i, c], col_s.at[n_c2 + i * E : n_c2 + (i + 1) * E]))
        lo, hi = (rows - 2, 0) if flip else (0, rows - 2)
        r = pick("row", hi, lo)
        for k in range(2):
            copies.append((one.at[r + k], row_s.at[k * cols : (k + 1) * cols]))
        lo, hi = (rows - 1, 0) if flip else (0, rows - 1)
        copies.append((two.at[pick("row", hi, lo)], row_s.at[t0 : t0 + cols]))
    copies.append((bias_one, b_one))
    copies.append((bias_two, b_two))
    started = [pltpu.make_async_copy(s, d, sems.at[i]) for i, (s, d) in enumerate(copies)]
    for c in started:
        c.start()
    for c in started[:n_first]:
        c.wait()
    for i in range(crows):
        p = (jnp.dot(latent_v[i], weight_v[...], preferred_element_type=F32) + bias_v[...]).astype(BF)
        proj[i] = p
        act[i] = silu(p.astype(F32)).astype(BF)
    for row_s, col_s, flip in sends:
        lo, hi = (crows - 1, 0) if flip else (0, crows - 1)
        row_s[2 * cols : t0, :] = act[pick("row", hi, lo)]
        lo, hi = (ccols - E, 0) if flip else (0, ccols - E)
        c = pl.ds(pick("col", hi, lo, E), E)
        for i in range(crows):
            col_s[n_c1 + i * E : n_c1 + (i + 1) * E, :] = act[i, c, :]
    for c in started[n_first:]:
        c.wait()


def corner_kernel(rows, crows, got_0, got_1, merged, act_edge, cor_0, cor_1):
    is_even = even("col")
    for i in range(2 * rows + crows):
        x, y = (g[i * E : (i + 1) * E, :].astype(F32) for g in (got_0, got_1))
        both = jnp.concatenate([jnp.where(is_even, x, y), jnp.where(is_even, y, x)], axis=0)
        merged[i * B : (i + 1) * B, :] = both.astype(BF)
        if rows <= i < rows + crows:
            act_edge[(i - rows) * B : (i - rows + 1) * B, :] = spread_edge(both)
    lows = (0, 1, rows, rows + crows)
    highs = (rows - 2, rows - 1, rows + crows - 1, 2 * rows + crows - 1)
    for k, (lo, hi) in enumerate(zip(lows, highs)):
        s = slice(k * B, (k + 1) * B)
        cor_0[s, :] = merged[pl.ds(pick("row", hi * B, lo * B, B), B), :]
        cor_1[s, :] = merged[pl.ds(pick("row", lo * B, hi * B, B), B), :]


def block(ref, i):
    return ref[i * B : (i + 1) * B, :].astype(F32)


def spread_edge(m):
    return jnp.where(
        low_half(), jnp.broadcast_to(m[0:1], (B, 128)), jnp.broadcast_to(m[B - 1 : B], (B, 128))
    ).astype(BF)


def put_row(dst, i, inside, edges):
    cols = dst.shape[1] - 2 * B
    dst[i, 0:B, :] = edges
    dst[i, B : B + cols, :] = inside
    dst[i, B + cols :, :] = edges


def conv_rows(frames, steps, weight, k, sums, slot):
    span = sums.shape[1] - 16
    w01, w2 = [], []
    zero = jnp.zeros(weight.shape[3:], BF)
    for a in steps:
        for p in range(4):
            if p < 3:
                w01.append(jnp.concatenate([weight[a, p, 0], weight[a, p, 1]], axis=1))
            w2.append(jnp.concatenate([weight[a, p, 2] if p < 3 else zero, weight[a, p - 1, 2] if p else zero], axis=1))
    w01, w2 = jnp.concatenate(w01, axis=0), jnp.concatenate(w2, axis=0)
    lhs = jnp.concatenate([f(k + p) for f in frames for p in range(4)], axis=1)
    y2 = jnp.dot(lhs, w2, preferred_element_type=F32)
    results = []
    for h in range(2):
        lhs = jnp.concatenate([f(k + h + p) for f in frames for p in range(3)], axis=1)
        y01 = jnp.dot(lhs, w01, preferred_element_type=F32)
        s = 2 * slot + h
        sums[s, 8 : 8 + span, 0:128] = y01[:, 0:128]
        sums[s, 8 : 8 + span, 128:256] = y2[:, h * 128 : (h + 1) * 128]
        results.append(sums[s, 7 : 7 + span, 0:128] + y01[:, 128:256] + sums[s, 9 : 9 + span, 128:256])
    return results


def joined(core, border):
    core, n = core
    return lambda i: border(i) if i < 2 else core(i - 2) if i < n + 2 else border(i - n)


def framed(tile, edges, first=0, each=1):
    def row(i):
        i = i // each
        e = edges[first + i * B : first + (i + 1) * B, :]
        return jnp.concatenate([e, tile[i], e], axis=0)

    return row, tile.shape[0] * each


def fill_kernel(one, act, act_up, send):
    rows, cols, _ = one.shape
    crows, ccols, _ = act.shape
    spread = spread_matrix(cols, ccols)
    for m in range(0, crows, 2):
        wide = jnp.dot(spread, jnp.concatenate([act[m], act[m + 1]], axis=1), preferred_element_type=F32).astype(BF)
        for h in range(2):
            act_up[m + h] = wide[:, h * 128 : (h + 1) * 128]
    lead = lax.axis_index("frm") == 0

    @pl.when(lead)
    def _():
        for i in range(rows):
            send[i] = act_up[i // 2]

    @pl.when(jnp.logical_not(lead))
    def _():
        send[...] = one[...]


def inner_kernel(one, act_up, merged, act_edge, weight, part, sums):
    frames = [joined(f, None) for f in (framed(one, merged), framed(act_up, act_edge, each=2))]
    for n, k in enumerate(range(2, 2 + part.shape[0], 2)):
        for h, v in enumerate(conv_rows(frames, (0, 2), weight, k, sums, n % 2)):
            part[k - 2 + h] = v


def border_kernel(row_0, row_1, cor_0, cor_1, merged, act_edge, cache_border, act_border, send):
    _, span, _ = cache_border.shape
    cols = span - 2 * B
    ccols = row_0.shape[0] - 3 * cols
    for lead in (True, False):

        @pl.when(even("row") == lead)
        def _(lead=lead):
            pairs = ((row_1, cor_1), (row_0, cor_0)) if lead else ((row_0, cor_0), (row_1, cor_1))
            coarse = jnp.concatenate([row[2 * cols : 2 * cols + ccols, :] for row, _ in pairs], axis=1)
            wide = jnp.dot(spread_matrix(cols, ccols), coarse, preferred_element_type=F32).astype(BF)
            for h, (row, cor) in enumerate(pairs):
                for k in range(2):
                    put_row(cache_border, 2 * h + k, row[k * cols : (k + 1) * cols, :], cor[k * B : (k + 1) * B, :])
                put_row(act_border, h, wide[:, h * 128 : (h + 1) * 128], spread_edge(block(cor, 2)))

    lead = lax.axis_index("frm") == 0
    n_edge = send.shape[0] - 4 * span

    @pl.when(lead)
    def _():
        for i in range(4):
            send[i * span : (i + 1) * span, :] = act_border[i // 2]
        for i in range(n_edge // B):
            send[4 * span + i * B : 4 * span + (i + 1) * B, :] = act_edge[i // 2 * B : (i // 2 + 1) * B, :]

    @pl.when(jnp.logical_not(lead))
    def _():
        for i in range(4):
            send[i * span : (i + 1) * span, :] = cache_border[i]
        send[4 * span :, :] = merged[0:n_edge, :]


def outer_kernel(
    one, act_up, merged, act_edge, cache_border, act_border, weight, two, row_0, row_1, cor_0, cor_1,
    part, two_frame, sums, *, first,
):
    rows, cols, _ = two.shape
    frames = (
        joined(framed(one, merged), lambda i: cache_border[i]),
        joined(framed(act_up, act_edge, each=2), lambda i: act_border[i // 2]),
    )
    for n, k in enumerate((0, rows)):
        for h, v in enumerate(conv_rows(frames, (0, 2), weight, k, sums, n)):
            part[2 * n + h] = v
    t0 = row_0.shape[0] - cols
    for i in range(rows):
        put_row(two_frame, i + 1, two[i], merged[(first + i) * B : (first + i + 1) * B, :])
    for lead in (True, False):

        @pl.when(even("row") == lead)
        def _(lead=lead):
            put_row(two_frame, rows + 1 if lead else 0, row_0[t0:, :], cor_0[3 * B :, :])
            put_row(two_frame, 0 if lead else rows + 1, row_1[t0:, :], cor_1[3 * B :, :])


def finish_row(out, i, v, row, n_out):
    span = v.shape[0]
    t = lax.broadcasted_iota(jnp.int32, (B, 128), 0)
    keep_left = (t != B - 1) | (lax.axis_index("col") != 0)
    keep_right = (t != 0) | (lax.axis_index("col") != lax.axis_size("col") - 1)
    v = silu(v)
    if row == 0:
        v = jnp.where(lax.axis_index("row") != 0, v, 0.0)
    if row == n_out - 1:
        v = jnp.where(lax.axis_index("row") != lax.axis_size("row") - 1, v, 0.0)
    out[i, 0:B, :] = jnp.where(keep_left, v[0:B], 0.0).astype(BF)
    out[i, B : span - B, :] = v[B : span - B].astype(BF)
    out[i, span - B :, :] = jnp.where(keep_right, v[span - B :], 0.0).astype(BF)


def middle_kernel(core, border, part_in, part_out, weight, bias, two_frame, out, send, sums):
    n_out, span, _ = out.shape
    frame = joined(framed(core, border, 4 * span), lambda i: border[i * span : (i + 1) * span, :])
    for k in range(0, n_out, 2):
        for h, v in enumerate(conv_rows((frame,), (1,), weight, k, sums, k // 2 % 2)):
            i = k + h
            part = part_in[i - 2] if 2 <= i < n_out - 2 else part_out[i if i < 2 else i - n_out + 4]
            finish_row(out, i, v + part + bias[...], i, n_out)
    for first, src in ((True, out), (False, two_frame)):

        @pl.when((lax.axis_index("frm") == 0) == first)
        def _(src=src):
            send[...] = src[...]


def own_two_kernel(two_frame, act_two, weight, proj, bias, part, sums):
    n_out, cols, _ = part.shape
    spread = spread_matrix(cols, proj.shape[1])
    frames = (lambda i: two_frame[i], lambda i: act_two[i])
    for k in range(0, n_out, 2):
        if k % 4 == 0:
            wide = jnp.dot(spread, jnp.concatenate([proj[k // 2], proj[k // 2 + 1]], axis=1), preferred_element_type=F32)
        base = wide[:, k % 4 * 64 : k % 4 * 64 + 128] + bias[...]
        for h, v in enumerate(conv_rows(frames, (0, 2), weight, k, sums, k // 2 % 2)):
            part[k + h] = v[B : B + cols] + base


def middle_two_kernel(middle, part, weight, out, sums, done, sems):
    n_out, cols, _ = done.shape
    copies = []
    for k in range(0, n_out, 2):
        for h, v in enumerate(conv_rows((lambda i: middle[i],), (1,), weight, k, sums, k // 2 % 2)):
            done[k + h] = (part[k + h] + v[B : B + cols]).astype(BF)
        copies.append(pltpu.make_async_copy(done.at[k : k + 2], out.at[k : k + 2], sems.at[k // 2]))
        copies[-1].start()
    for c in copies:
        c.wait()


def exchange(x, axis, first):
    pairs = [(i, i + 1) for i in range(first, lax.axis_size(axis) - 1, 2)]
    return lax.ppermute(x, axis, pairs + [(j, i) for i, j in pairs])


def swap(x):
    return lax.ppermute(x, "frm", [(0, 1), (1, 0)])


def program(latent, proj_weight, proj_bias, cache_one, cache_two, conv_one, bias_one, conv_two, bias_two):
    latent, one, two = latent[0], cache_one[0], cache_two[0]
    rows, cols, ch = one.shape
    crows, ccols, lch = latent.shape
    span = cols + 2 * B
    n_edge = (2 * rows + crows) * B
    n_send = (2 * rows + crows) * E
    n_row = 3 * cols + ccols
    sums = pltpu.VMEM((4, span + 16, 2 * ch), F32)
    proj, act, row_0, row_1, col_0, col_1, b_one, b_two = call(
        first_kernel,
        [
            ((crows, ccols, ch), BF),
            ((crows, ccols, ch), BF),
            ((n_row, ch), BF),
            ((n_row, ch), BF),
            ((n_send, ch), BF),
            ((n_send, ch), BF),
            ((1, ch), F32),
            ((1, ch), F32),
        ],
        [HBM] * 7,
        scratch=[
            pltpu.VMEM((crows, ccols, lch), BF),
            pltpu.VMEM((lch, ch), BF),
            pltpu.VMEM((1, ch), F32),
            pltpu.SemaphoreType.DMA((3 + 4 * rows + 8,)),
        ],
        flops=10**8,
        nbytes=2 * 10**6,
        limit=24,
    )(latent, proj_weight, proj_bias.reshape(1, ch), one, two, bias_one.reshape(1, ch), bias_two.reshape(1, ch))
    got_1 = exchange(col_1, "col", 1)
    got_0 = exchange(col_0, "col", 0)
    row_1 = exchange(row_1, "row", 1)
    row_0 = exchange(row_0, "row", 0)
    third = 2 * 9 * ch * ch * rows * cols
    act_up, send_core = call(
        fill_kernel, [((crows, cols, ch), BF), ((rows, cols, ch), BF)], [VMEM] * 2, flops=10**8, nbytes=4 * 10**6
    )(one, act)
    middle_core = swap(send_core)
    merged, act_edge, cor_0, cor_1 = call(
        functools.partial(corner_kernel, rows, crows),
        [((n_edge, ch), BF), ((crows * B, ch), BF), ((4 * B, ch), BF), ((4 * B, ch), BF)],
        [VMEM] * 2,
        flops=10**6,
        nbytes=2 * 10**5,
    )(got_0, got_1)
    cor_0 = exchange(cor_0, "row", 0)
    cor_1 = exchange(cor_1, "row", 1)
    (part_in,) = call(
        inner_kernel, [((rows - 2, span, ch), F32)], [VMEM] * 5, scratch=[sums], flops=2 * third, nbytes=4 * 10**6
    )(one, act_up, merged, act_edge, conv_one)
    cache_border, act_border, send_border = call(
        border_kernel,
        [((4, span, ch), BF), ((2, span, ch), BF), ((4 * span + rows * B, ch), BF)],
        [VMEM] * 6,
        flops=10**8,
        nbytes=4 * 10**6,
    )(row_0, row_1, cor_0, cor_1, merged, act_edge)
    middle_border = swap(send_border)
    part_out, two_frame = call(
        functools.partial(outer_kernel, first=rows + crows),
        [((4, span, ch), F32), ((rows + 2, span, ch), BF)],
        [VMEM] * 12,
        scratch=[sums],
        flops=third,
        nbytes=4 * 10**6,
    )(one, act_up, merged, act_edge, cache_border, act_border, conv_one, two, row_0, row_1, cor_0, cor_1)
    act_two, send_two = call(
        middle_kernel, [((rows + 2, span, ch), BF)] * 2, [VMEM] * 7, scratch=[sums], flops=third, nbytes=6 * 10**6
    )(middle_core, middle_border, part_in, part_out, conv_one, b_one, two_frame)
    middle_two = swap(send_two)
    (part_two,) = call(
        own_two_kernel, [((rows, cols, ch), F32)], [VMEM] * 5, scratch=[sums], flops=2 * third, nbytes=6 * 10**6
    )(two_frame, act_two, conv_two, proj, b_two)
    (decoded,) = call(
        middle_two_kernel,
        [((rows, cols, ch), BF)],
        [VMEM] * 3,
        scratch=[sums, pltpu.VMEM((rows, cols, ch), BF), pltpu.SemaphoreType.DMA((rows // 2,))],
        out_specs=[HBM],
        flops=third,
        nbytes=6 * 10**6,
    )(middle_two, part_two, conv_two)
    return decoded[None]


def solution(mesh):
    placed = (
        P(("grp", "frm"), "row", "col", None),
        P(),
        P(),
        P(("grp", "frm"), "row", "col", None),
        P(("grp", "frm"), "row", "col", None),
        P(),
        P(),
        P(),
        P(),
    )
    return jax.shard_map(
        program,
        mesh=mesh,
        in_specs=placed,
        out_specs=P(("grp", "frm"), "row", "col", None),
        check_vma=False,
    )
```

```python
import functools

import jax
import jax.numpy as jnp
from jax import lax
from jax.experimental import pallas as pl
from jax.experimental.pallas import tpu as pltpu
from jax.sharding import PartitionSpec as P

B = 16
E = B // 2
BF = jnp.bfloat16
F32 = jnp.float32
VMEM = pl.BlockSpec(memory_space=pltpu.VMEM)
HBM = pl.BlockSpec(memory_space=pltpu.HBM)


def call(body, outs, specs, scratch=(), flops=0, nbytes=0, limit=24, out_specs=None):
    run = pl.pallas_call(
        body,
        out_shape=[jax.ShapeDtypeStruct(s, d) for s, d in outs],
        in_specs=specs,
        out_specs=out_specs or [VMEM] * len(outs),
        scratch_shapes=list(scratch),
        cost_estimate=pl.CostEstimate(flops=flops, bytes_accessed=nbytes, transcendentals=0),
        compiler_params=pltpu.CompilerParams(vmem_limit_bytes=int(limit * 1024 * 1024)),
    )
    held = lambda v, spec: pltpu.with_memory_space_constraint(v, pltpu.HBM) if spec is HBM else v
    return lambda *args: run(*(held(v, spec) for v, spec in zip(args, specs, strict=True)))


def silu(v):
    return v / (1.0 + jnp.exp(-v))


def low_half():
    return lax.broadcasted_iota(jnp.int32, (B, 128), 0) < B // 2


def spread_matrix(cols, ccols):
    fine = lax.broadcasted_iota(jnp.int32, (cols, ccols), 0)
    return (fine // 2 == lax.broadcasted_iota(jnp.int32, (cols, ccols), 1)).astype(F32).astype(BF)


def even(axis):
    return lax.rem(lax.axis_index(axis), 2) == 0


def pick(axis, high, low, step=1):
    start = jnp.where(even(axis), high, low)
    return pl.multiple_of(start, step) if step > 1 else start


def first_kernel(
    latent, weight, bias, one, two, bias_one, bias_two,
    proj, act, row_0, row_1, col_0, col_1, b_one, b_two,
    latent_v, weight_v, bias_v, sems,
):
    rows, cols, _ = one.shape
    crows, ccols, _ = latent.shape
    copies = [(latent, latent_v), (weight, weight_v), (bias, bias_v)]
    n_first = len(copies)
    t0 = 2 * cols + ccols
    sends = ((row_0, col_0, False), (row_1, col_1, True))
    for row_s, col_s, flip in sends:
        lo, hi = (cols - E, 0) if flip else (0, cols - E)
        c = pl.ds(pick("col", hi, lo, E), E)
        copies.append((one.at[:, c], col_s.at[0:rows]))
        copies.append((two.at[:, c], col_s.at[rows + crows :]))
        lo, hi = (rows - 2, 0) if flip else (0, rows - 2)
        r = pick("row", hi, lo)
        for k in range(2):
            copies.append((one.at[r + k], row_s.at[k * cols : (k + 1) * cols]))
        lo, hi = (rows - 1, 0) if flip else (0, rows - 1)
        copies.append((two.at[pick("row", hi, lo)], row_s.at[t0 : t0 + cols]))
    copies.append((bias_one, b_one))
    copies.append((bias_two, b_two))
    started = [pltpu.make_async_copy(s, d, sems.at[i]) for i, (s, d) in enumerate(copies)]
    for c in started:
        c.start()
    for c in started[:n_first]:
        c.wait()
    for i in range(crows):
        p = (jnp.dot(latent_v[i], weight_v[...], preferred_element_type=F32) + bias_v[...]).astype(BF)
        proj[i] = p
        act[i] = silu(p.astype(F32)).astype(BF)
    for row_s, col_s, flip in sends:
        lo, hi = (crows - 1, 0) if flip else (0, crows - 1)
        row_s[2 * cols : t0, :] = act[pick("row", hi, lo)]
        lo, hi = (ccols - E, 0) if flip else (0, ccols - E)
        c = pl.ds(pick("col", hi, lo, E), E)
        for i in range(crows):
            col_s[rows + i] = act[i, c, :]
    for c in started[n_first:]:
        c.wait()


def corner_kernel(rows, crows, got_0, got_1, merged, act_edge, cor_0, cor_1):
    is_even = even("col")
    for i in range(2 * rows + crows):
        x, y = (g[i].astype(F32) for g in (got_0, got_1))
        both = jnp.concatenate([jnp.where(is_even, x, y), jnp.where(is_even, y, x)], axis=0)
        merged[i * B : (i + 1) * B, :] = both.astype(BF)
        if rows <= i < rows + crows:
            act_edge[(i - rows) * B : (i - rows + 1) * B, :] = spread_edge(both)
    lows = (0, 1, rows, rows + crows)
    highs = (rows - 2, rows - 1, rows + crows - 1, 2 * rows + crows - 1)
    for k, (lo, hi) in enumerate(zip(lows, highs)):
        s = slice(k * B, (k + 1) * B)
        cor_0[s, :] = merged[pl.ds(pick("row", hi * B, lo * B, B), B), :]
        cor_1[s, :] = merged[pl.ds(pick("row", lo * B, hi * B, B), B), :]


def block(ref, i):
    return ref[i * B : (i + 1) * B, :].astype(F32)


def spread_edge(m):
    return jnp.where(
        low_half(), jnp.broadcast_to(m[0:1], (B, 128)), jnp.broadcast_to(m[B - 1 : B], (B, 128))
    ).astype(BF)


def put_row(dst, i, inside, edges):
    cols = dst.shape[1] - 2 * B
    dst[i, 0:B, :] = edges
    dst[i, B : B + cols, :] = inside
    dst[i, B + cols :, :] = edges


def conv_rows(frames, steps, weight, k, sums, slot):
    span = sums.shape[1] - 16
    w01, w2 = [], []
    zero = jnp.zeros(weight.shape[3:], BF)
    for a in steps:
        for p in range(4):
            if p < 3:
                w01.append(jnp.concatenate([weight[a, p, 0], weight[a, p, 1]], axis=1))
            w2.append(jnp.concatenate([weight[a, p, 2] if p < 3 else zero, weight[a, p - 1, 2] if p else zero], axis=1))
    w01, w2 = jnp.concatenate(w01, axis=0), jnp.concatenate(w2, axis=0)
    lhs = jnp.concatenate([f(k + p) for f in frames for p in range(4)], axis=1)
    y2 = jnp.dot(lhs, w2, preferred_element_type=F32)
    results = []
    for h in range(2):
        lhs = jnp.concatenate([f(k + h + p) for f in frames for p in range(3)], axis=1)
        y01 = jnp.dot(lhs, w01, preferred_element_type=F32)
        s = 2 * slot + h
        sums[s, 8 : 8 + span, 0:128] = y01[:, 0:128]
        sums[s, 8 : 8 + span, 128:256] = y2[:, h * 128 : (h + 1) * 128]
        results.append(sums[s, 7 : 7 + span, 0:128] + y01[:, 128:256] + sums[s, 9 : 9 + span, 128:256])
    return results


def joined(core, border):
    core, n = core
    return lambda i: border(i) if i < 2 else core(i - 2) if i < n + 2 else border(i - n)


def framed(tile, edges, first=0, each=1):
    def row(i):
        i = i // each
        e = edges[first + i * B : first + (i + 1) * B, :]
        return jnp.concatenate([e, tile[i], e], axis=0)

    return row, tile.shape[0] * each


def fill_kernel(act, act_up):
    crows, cols, _ = act_up.shape
    ccols = act.shape[1]
    spread = spread_matrix(cols, ccols)
    for m in range(0, crows, 2):
        wide = jnp.dot(spread, jnp.concatenate([act[m], act[m + 1]], axis=1), preferred_element_type=F32).astype(BF)
        for h in range(2):
            act_up[m + h] = wide[:, h * 128 : (h + 1) * 128]


def inner_kernel(one, act_up, merged, act_edge, weight, part, sums):
    frames = [joined(f, None) for f in (framed(one, merged), framed(act_up, act_edge, each=2))]
    for n, k in enumerate(range(2, 2 + part.shape[0], 2)):
        for h, v in enumerate(conv_rows(frames, (0, 2), weight, k, sums, n % 2)):
            part[k - 2 + h] = v


def border_kernel(one, act_up, merged, act_edge, row_0, row_1, cor_0, cor_1, cache_border, act_border, send):
    rows, cols, _ = one.shape
    ccols = row_0.shape[0] - 3 * cols
    for even_row in (True, False):

        @pl.when(even("row") == even_row)
        def _(even_row=even_row):
            pairs = ((row_1, cor_1), (row_0, cor_0)) if even_row else ((row_0, cor_0), (row_1, cor_1))
            coarse = jnp.concatenate([row[2 * cols : 2 * cols + ccols, :] for row, _ in pairs], axis=1)
            wide = jnp.dot(spread_matrix(cols, ccols), coarse, preferred_element_type=F32).astype(BF)
            for h, (row, cor) in enumerate(pairs):
                for k in range(2):
                    put_row(cache_border, 2 * h + k, row[k * cols : (k + 1) * cols, :], cor[k * B : (k + 1) * B, :])
                put_row(act_border, h, wide[:, h * 128 : (h + 1) * 128], spread_edge(block(cor, 2)))

    lead = lax.axis_index("frm") == 0

    @pl.when(lead)
    def _():
        for i in range(4):
            send[i if i < 2 else rows + i] = act_border[i // 2]
        for i in range(rows):
            m = i // 2
            put_row(send, i + 2, act_up[m], act_edge[m * B : (m + 1) * B, :])

    @pl.when(jnp.logical_not(lead))
    def _():
        for i in range(4):
            send[i if i < 2 else rows + i] = cache_border[i]
        for i in range(rows):
            put_row(send, i + 2, one[i], merged[i * B : (i + 1) * B, :])


def outer_kernel(
    one, act_up, merged, act_edge, cache_border, act_border, weight, two, row_0, row_1, cor_0, cor_1,
    part, two_frame, sums, *, first,
):
    rows, cols, _ = two.shape
    frames = (
        joined(framed(one, merged), lambda i: cache_border[i]),
        joined(framed(act_up, act_edge, each=2), lambda i: act_border[i // 2]),
    )
    for n, k in enumerate((0, rows)):
        for h, v in enumerate(conv_rows(frames, (0, 2), weight, k, sums, n)):
            part[2 * n + h] = v
    t0 = row_0.shape[0] - cols
    for i in range(rows):
        put_row(two_frame, i + 1, two[i], merged[(first + i) * B : (first + i + 1) * B, :])
    for lead in (True, False):

        @pl.when(even("row") == lead)
        def _(lead=lead):
            put_row(two_frame, rows + 1 if lead else 0, row_0[t0:, :], cor_0[3 * B :, :])
            put_row(two_frame, 0 if lead else rows + 1, row_1[t0:, :], cor_1[3 * B :, :])


def finish_row(out, i, v, row, n_out):
    span = v.shape[0]
    t = lax.broadcasted_iota(jnp.int32, (B, 128), 0)
    keep_left = (t != B - 1) | (lax.axis_index("col") != 0)
    keep_right = (t != 0) | (lax.axis_index("col") != lax.axis_size("col") - 1)
    v = silu(v)
    if row == 0:
        v = jnp.where(lax.axis_index("row") != 0, v, 0.0)
    if row == n_out - 1:
        v = jnp.where(lax.axis_index("row") != lax.axis_size("row") - 1, v, 0.0)
    out[i, 0:B, :] = jnp.where(keep_left, v[0:B], 0.0).astype(BF)
    out[i, B : span - B, :] = v[B : span - B].astype(BF)
    out[i, span - B :, :] = jnp.where(keep_right, v[span - B :], 0.0).astype(BF)


def middle_kernel(middle, part_in, part_out, weight, bias, two_frame, out, send, sums):
    n_out, _, _ = out.shape
    for k in range(0, n_out, 2):
        for h, v in enumerate(conv_rows((lambda i: middle[i],), (1,), weight, k, sums, k // 2 % 2)):
            i = k + h
            part = part_in[i - 2] if 2 <= i < n_out - 2 else part_out[i if i < 2 else i - n_out + 4]
            finish_row(out, i, v + part + bias[...], i, n_out)
    for first, src in ((True, out), (False, two_frame)):

        @pl.when((lax.axis_index("frm") == 0) == first)
        def _(src=src):
            send[...] = src[...]


def own_two_kernel(two_frame, act_two, weight, proj, bias, part, sums):
    n_out, cols, _ = part.shape
    spread = spread_matrix(cols, proj.shape[1])
    frames = (lambda i: two_frame[i], lambda i: act_two[i])
    for k in range(0, n_out, 2):
        if k % 4 == 0:
            wide = jnp.dot(spread, jnp.concatenate([proj[k // 2], proj[k // 2 + 1]], axis=1), preferred_element_type=F32)
        base = wide[:, k % 4 * 64 : k % 4 * 64 + 128] + bias[...]
        for h, v in enumerate(conv_rows(frames, (0, 2), weight, k, sums, k // 2 % 2)):
            part[k + h] = v[B : B + cols] + base


def middle_two_kernel(middle, part, weight, out, sums, done, sems):
    n_out, cols, _ = done.shape
    copies = []
    for k in range(0, n_out, 2):
        for h, v in enumerate(conv_rows((lambda i: middle[i],), (1,), weight, k, sums, k // 2 % 2)):
            done[k + h] = (part[k + h] + v[B : B + cols]).astype(BF)
        copies.append(pltpu.make_async_copy(done.at[k : k + 2], out.at[k : k + 2], sems.at[k // 2]))
        copies[-1].start()
    for c in copies:
        c.wait()


def exchange(x, axis, first):
    pairs = [(i, i + 1) for i in range(first, lax.axis_size(axis) - 1, 2)]
    return lax.ppermute(x, axis, pairs + [(j, i) for i, j in pairs])


def swap(x):
    return lax.ppermute(x, "frm", [(0, 1), (1, 0)])


def program(latent, proj_weight, proj_bias, cache_one, cache_two, conv_one, bias_one, conv_two, bias_two):
    latent, one, two = latent[0], cache_one[0], cache_two[0]
    rows, cols, ch = one.shape
    crows, ccols, lch = latent.shape
    span = cols + 2 * B
    n_edge = (2 * rows + crows) * B
    col_shape = (2 * rows + crows, E, ch)
    n_row = 3 * cols + ccols
    sums = pltpu.VMEM((4, span + 16, 2 * ch), F32)
    proj, act, row_0, row_1, col_0, col_1, b_one, b_two = call(
        first_kernel,
        [
            ((crows, ccols, ch), BF),
            ((crows, ccols, ch), BF),
            ((n_row, ch), BF),
            ((n_row, ch), BF),
            (col_shape, BF),
            (col_shape, BF),
            ((1, ch), F32),
            ((1, ch), F32),
        ],
        [HBM] * 7,
        scratch=[
            pltpu.VMEM((crows, ccols, lch), BF),
            pltpu.VMEM((lch, ch), BF),
            pltpu.VMEM((1, ch), F32),
            pltpu.SemaphoreType.DMA((15,)),
        ],
        flops=10**8,
        nbytes=2 * 10**6,
        limit=24,
    )(latent, proj_weight, proj_bias.reshape(1, ch), one, two, bias_one.reshape(1, ch), bias_two.reshape(1, ch))
    got_1 = exchange(col_1, "col", 1)
    got_0 = exchange(col_0, "col", 0)
    row_1 = exchange(row_1, "row", 1)
    row_0 = exchange(row_0, "row", 0)
    third = 2 * 9 * ch * ch * rows * cols
    (act_up,) = call(fill_kernel, [((crows, cols, ch), BF)], [VMEM], flops=10**8, nbytes=10**6)(act)
    merged, act_edge, cor_0, cor_1 = call(
        functools.partial(corner_kernel, rows, crows),
        [((n_edge, ch), BF), ((crows * B, ch), BF), ((4 * B, ch), BF), ((4 * B, ch), BF)],
        [VMEM] * 2,
        flops=10**6,
        nbytes=2 * 10**5,
    )(got_0, got_1)
    cor_0 = exchange(cor_0, "row", 0)
    cor_1 = exchange(cor_1, "row", 1)
    (part_in,) = call(
        inner_kernel, [((rows - 2, span, ch), F32)], [VMEM] * 5, scratch=[sums], flops=2 * third, nbytes=4 * 10**6
    )(one, act_up, merged, act_edge, conv_one)
    cache_border, act_border, send = call(
        border_kernel,
        [((4, span, ch), BF), ((2, span, ch), BF), ((rows + 4, span, ch), BF)],
        [VMEM] * 8,
        flops=10**8,
        nbytes=4 * 10**6,
    )(one, act_up, merged, act_edge, row_0, row_1, cor_0, cor_1)
    middle = swap(send)
    part_out, two_frame = call(
        functools.partial(outer_kernel, first=rows + crows),
        [((4, span, ch), F32), ((rows + 2, span, ch), BF)],
        [VMEM] * 12,
        scratch=[sums],
        flops=third,
        nbytes=4 * 10**6,
    )(one, act_up, merged, act_edge, cache_border, act_border, conv_one, two, row_0, row_1, cor_0, cor_1)
    act_two, send_two = call(
        middle_kernel, [((rows + 2, span, ch), BF)] * 2, [VMEM] * 6, scratch=[sums], flops=third, nbytes=6 * 10**6
    )(middle, part_in, part_out, conv_one, b_one, two_frame)
    middle_two = swap(send_two)
    (part_two,) = call(
        own_two_kernel, [((rows, cols, ch), F32)], [VMEM] * 5, scratch=[sums], flops=2 * third, nbytes=6 * 10**6
    )(two_frame, act_two, conv_two, proj, b_two)
    (decoded,) = call(
        middle_two_kernel,
        [((rows, cols, ch), BF)],
        [VMEM] * 3,
        scratch=[sums, pltpu.VMEM((rows, cols, ch), BF), pltpu.SemaphoreType.DMA((rows // 2,))],
        out_specs=[HBM],
        flops=third,
        nbytes=6 * 10**6,
    )(middle_two, part_two, conv_two)
    return decoded[None]


def solution(mesh):
    placed = (
        P(("grp", "frm"), "row", "col", None),
        P(),
        P(),
        P(("grp", "frm"), "row", "col", None),
        P(("grp", "frm"), "row", "col", None),
        P(),
        P(),
        P(),
        P(),
    )
    return jax.shard_map(
        program,
        mesh=mesh,
        in_specs=placed,
        out_specs=P(("grp", "frm"), "row", "col", None),
        check_vma=False,
    )
```

```python
import functools

import jax
import jax.numpy as jnp
from jax import lax
from jax.experimental import pallas as pl
from jax.experimental.pallas import tpu as pltpu
from jax.sharding import PartitionSpec as P

B = 16
E = B // 2
BF = jnp.bfloat16
F32 = jnp.float32
VMEM = pl.BlockSpec(memory_space=pltpu.VMEM)
HBM = pl.BlockSpec(memory_space=pltpu.HBM)


def call(body, outs, specs, scratch=(), flops=0, nbytes=0, limit=24, out_specs=None):
    run = pl.pallas_call(
        body,
        out_shape=[jax.ShapeDtypeStruct(s, d) for s, d in outs],
        in_specs=specs,
        out_specs=out_specs or [VMEM] * len(outs),
        scratch_shapes=list(scratch),
        cost_estimate=pl.CostEstimate(flops=flops, bytes_accessed=nbytes, transcendentals=0),
        compiler_params=pltpu.CompilerParams(vmem_limit_bytes=int(limit * 1024 * 1024)),
    )
    held = lambda v, spec: pltpu.with_memory_space_constraint(v, pltpu.HBM) if spec is HBM else v
    return lambda *args: run(*(held(v, spec) for v, spec in zip(args, specs, strict=True)))


def silu(v):
    return v / (1.0 + jnp.exp(-v))


def low_half():
    return lax.broadcasted_iota(jnp.int32, (B, 128), 0) < B // 2


def spread_matrix(cols, ccols):
    fine = lax.broadcasted_iota(jnp.int32, (cols, ccols), 0)
    return (fine // 2 == lax.broadcasted_iota(jnp.int32, (cols, ccols), 1)).astype(F32).astype(BF)


def even(axis):
    return lax.rem(lax.axis_index(axis), 2) == 0


def pick(axis, high, low, step=1):
    start = jnp.where(even(axis), high, low)
    return pl.multiple_of(start, step) if step > 1 else start


def first_kernel(
    latent, weight, bias, one, two, bias_one, bias_two,
    proj, act, row_0, row_1, col_0, col_1, b_one, b_two,
    latent_v, weight_v, bias_v, sems,
):
    rows, cols, _ = one.shape
    crows, ccols, _ = latent.shape
    copies = [(latent, latent_v), (weight, weight_v), (bias, bias_v)]
    n_first = len(copies)
    t0 = 2 * cols + ccols
    sends = ((row_0, col_0, False), (row_1, col_1, True))
    for row_s, col_s, flip in sends:
        lo, hi = (cols - E, 0) if flip else (0, cols - E)
        c = pl.ds(pick("col", hi, lo, E), E)
        copies.append((one.at[:, c], col_s.at[0:rows]))
        copies.append((two.at[:, c], col_s.at[rows + crows :]))
        lo, hi = (rows - 2, 0) if flip else (0, rows - 2)
        r = pick("row", hi, lo)
        for k in range(2):
            copies.append((one.at[r + k], row_s.at[k * cols : (k + 1) * cols]))
        lo, hi = (rows - 1, 0) if flip else (0, rows - 1)
        copies.append((two.at[pick("row", hi, lo)], row_s.at[t0 : t0 + cols]))
    copies.append((bias_one, b_one))
    copies.append((bias_two, b_two))
    started = [pltpu.make_async_copy(s, d, sems.at[i]) for i, (s, d) in enumerate(copies)]
    for c in started:
        c.start()
    for c in started[:n_first]:
        c.wait()
    for i in range(crows):
        p = (jnp.dot(latent_v[i], weight_v[...], preferred_element_type=F32) + bias_v[...]).astype(BF)
        proj[i] = p
        act[i] = silu(p.astype(F32)).astype(BF)
    for row_s, col_s, flip in sends:
        lo, hi = (crows - 1, 0) if flip else (0, crows - 1)
        row_s[2 * cols : t0, :] = act[pick("row", hi, lo)]
        lo, hi = (ccols - E, 0) if flip else (0, ccols - E)
        c = pl.ds(pick("col", hi, lo, E), E)
        for i in range(crows):
            col_s[rows + i] = act[i, c, :]
    for c in started[n_first:]:
        c.wait()


def corner_kernel(rows, crows, got_0, got_1, merged, act_edge, cor_0, cor_1):
    is_even = even("col")
    for i in range(2 * rows + crows):
        x, y = (g[i].astype(F32) for g in (got_0, got_1))
        both = jnp.concatenate([jnp.where(is_even, x, y), jnp.where(is_even, y, x)], axis=0)
        merged[i * B : (i + 1) * B, :] = both.astype(BF)
        if rows <= i < rows + crows:
            act_edge[(i - rows) * B : (i - rows + 1) * B, :] = spread_edge(both)
    lows = (0, 1, rows, rows + crows)
    highs = (rows - 2, rows - 1, rows + crows - 1, 2 * rows + crows - 1)
    for k, (lo, hi) in enumerate(zip(lows, highs)):
        s = slice(k * B, (k + 1) * B)
        cor_0[s, :] = merged[pl.ds(pick("row", hi * B, lo * B, B), B), :]
        cor_1[s, :] = merged[pl.ds(pick("row", lo * B, hi * B, B), B), :]


def block(ref, i):
    return ref[i * B : (i + 1) * B, :].astype(F32)


def spread_edge(m):
    return jnp.where(
        low_half(), jnp.broadcast_to(m[0:1], (B, 128)), jnp.broadcast_to(m[B - 1 : B], (B, 128))
    ).astype(BF)


def put_row(dst, i, inside, edges):
    cols = dst.shape[1] - 2 * B
    dst[i, 0:B, :] = edges
    dst[i, B : B + cols, :] = inside
    dst[i, B + cols :, :] = edges


def conv_rows(frames, steps, weight, k, sums, slot):
    span = sums.shape[1] - 16
    w01, w2 = [], []
    zero = jnp.zeros(weight.shape[3:], BF)
    for a in steps:
        for p in range(4):
            if p < 3:
                w01.append(jnp.concatenate([weight[a, p, 0], weight[a, p, 1]], axis=1))
            w2.append(jnp.concatenate([weight[a, p, 2] if p < 3 else zero, weight[a, p - 1, 2] if p else zero], axis=1))
    w01, w2 = jnp.concatenate(w01, axis=0), jnp.concatenate(w2, axis=0)
    lhs = jnp.concatenate([f(k + p) for f in frames for p in range(4)], axis=1)
    y2 = jnp.dot(lhs, w2, preferred_element_type=F32)
    results = []
    for h in range(2):
        lhs = jnp.concatenate([f(k + h + p) for f in frames for p in range(3)], axis=1)
        y01 = jnp.dot(lhs, w01, preferred_element_type=F32)
        s = 2 * slot + h
        sums[s, 8 : 8 + span, 0:128] = y01[:, 0:128]
        sums[s, 8 : 8 + span, 128:256] = y2[:, h * 128 : (h + 1) * 128]
        results.append(sums[s, 7 : 7 + span, 0:128] + y01[:, 128:256] + sums[s, 9 : 9 + span, 128:256])
    return results


def shift_rows(frame, rows, moved):
    span = moved.shape[1]
    for i in rows:
        x = frame(i).astype(F32)
        moved[i, :, 0:128] = pltpu.roll(x, 1, 0).astype(BF)
        moved[i, :, 128:256] = pltpu.roll(x, span - 1, 0).astype(BF)


def conv_pair(frame, moved, step, weight, k):
    lhs, rhs = [], []
    zero = jnp.zeros(weight.shape[3:], BF)
    for p in range(4):
        lhs += [moved[k + p], frame(k + p)]
        for q in (0, 2, 1):
            first = weight[step, p, q] if p < 3 else zero
            second = weight[step, p - 1, q] if p else zero
            rhs.append(jnp.concatenate([first, second], axis=1))
    y = jnp.dot(jnp.concatenate(lhs, axis=1), jnp.concatenate(rhs, axis=0), preferred_element_type=F32)
    return y[:, 0:128], y[:, 128:256]


def joined(core, border):
    core, n = core
    return lambda i: border(i) if i < 2 else core(i - 2) if i < n + 2 else border(i - n)


def framed(tile, edges, first=0, each=1):
    def row(i):
        i = i // each
        e = edges[first + i * B : first + (i + 1) * B, :]
        return jnp.concatenate([e, tile[i], e], axis=0)

    return row, tile.shape[0] * each


def fill_kernel(act, act_up):
    crows, cols, _ = act_up.shape
    ccols = act.shape[1]
    spread = spread_matrix(cols, ccols)
    for m in range(0, crows, 2):
        wide = jnp.dot(spread, jnp.concatenate([act[m], act[m + 1]], axis=1), preferred_element_type=F32).astype(BF)
        for h in range(2):
            act_up[m + h] = wide[:, h * 128 : (h + 1) * 128]


def inner_kernel(one, act_up, merged, act_edge, weight, part, sums):
    frames = [joined(f, None) for f in (framed(one, merged), framed(act_up, act_edge, each=2))]
    for n, k in enumerate(range(2, 2 + part.shape[0], 2)):
        for h, v in enumerate(conv_rows(frames, (0, 2), weight, k, sums, n % 2)):
            part[k - 2 + h] = v


def border_kernel(one, act_up, merged, act_edge, row_0, row_1, cor_0, cor_1, cache_border, act_border, send):
    rows, cols, _ = one.shape
    ccols = row_0.shape[0] - 3 * cols
    for even_row in (True, False):

        @pl.when(even("row") == even_row)
        def _(even_row=even_row):
            pairs = ((row_1, cor_1), (row_0, cor_0)) if even_row else ((row_0, cor_0), (row_1, cor_1))
            coarse = jnp.concatenate([row[2 * cols : 2 * cols + ccols, :] for row, _ in pairs], axis=1)
            wide = jnp.dot(spread_matrix(cols, ccols), coarse, preferred_element_type=F32).astype(BF)
            for h, (row, cor) in enumerate(pairs):
                for k in range(2):
                    put_row(cache_border, 2 * h + k, row[k * cols : (k + 1) * cols, :], cor[k * B : (k + 1) * B, :])
                put_row(act_border, h, wide[:, h * 128 : (h + 1) * 128], spread_edge(block(cor, 2)))

    lead = lax.axis_index("frm") == 0

    @pl.when(lead)
    def _():
        for i in range(4):
            send[i if i < 2 else rows + i] = act_border[i // 2]
        for i in range(rows):
            m = i // 2
            put_row(send, i + 2, act_up[m], act_edge[m * B : (m + 1) * B, :])

    @pl.when(jnp.logical_not(lead))
    def _():
        for i in range(4):
            send[i if i < 2 else rows + i] = cache_border[i]
        for i in range(rows):
            put_row(send, i + 2, one[i], merged[i * B : (i + 1) * B, :])


def outer_kernel(
    one, act_up, merged, act_edge, cache_border, act_border, weight, two, row_0, row_1, cor_0, cor_1,
    part, two_frame, sums, *, first,
):
    rows, cols, _ = two.shape
    frames = (
        joined(framed(one, merged), lambda i: cache_border[i]),
        joined(framed(act_up, act_edge, each=2), lambda i: act_border[i // 2]),
    )
    for n, k in enumerate((0, rows)):
        for h, v in enumerate(conv_rows(frames, (0, 2), weight, k, sums, n)):
            part[2 * n + h] = v
    t0 = row_0.shape[0] - cols
    for i in range(rows):
        put_row(two_frame, i + 1, two[i], merged[(first + i) * B : (first + i + 1) * B, :])
    for lead in (True, False):

        @pl.when(even("row") == lead)
        def _(lead=lead):
            put_row(two_frame, rows + 1 if lead else 0, row_0[t0:, :], cor_0[3 * B :, :])
            put_row(two_frame, 0 if lead else rows + 1, row_1[t0:, :], cor_1[3 * B :, :])


def finish_row(out, i, v, row, n_out):
    span = v.shape[0]
    t = lax.broadcasted_iota(jnp.int32, (B, 128), 0)
    keep_left = (t != B - 1) | (lax.axis_index("col") != 0)
    keep_right = (t != 0) | (lax.axis_index("col") != lax.axis_size("col") - 1)
    v = silu(v)
    if row == 0:
        v = jnp.where(lax.axis_index("row") != 0, v, 0.0)
    if row == n_out - 1:
        v = jnp.where(lax.axis_index("row") != lax.axis_size("row") - 1, v, 0.0)
    out[i, 0:B, :] = jnp.where(keep_left, v[0:B], 0.0).astype(BF)
    out[i, B : span - B, :] = v[B : span - B].astype(BF)
    out[i, span - B :, :] = jnp.where(keep_right, v[span - B :], 0.0).astype(BF)


def middle_kernel(middle, part_in, part_out, weight, bias, two_frame, out, send, moved):
    n_out, _, _ = out.shape
    row = lambda i: middle[i]
    for k in range(0, n_out, 2):
        shift_rows(row, range(k + 2 if k else 0, k + 4), moved)
        for h, v in enumerate(conv_pair(row, moved, 1, weight, k)):
            i = k + h
            part = part_in[i - 2] if 2 <= i < n_out - 2 else part_out[i if i < 2 else i - n_out + 4]
            finish_row(out, i, v + part + bias[...], i, n_out)
    for first, src in ((True, out), (False, two_frame)):

        @pl.when((lax.axis_index("frm") == 0) == first)
        def _(src=src):
            send[...] = src[...]


def own_two_kernel(two_frame, act_two, weight, proj, bias, part, sums):
    n_out, cols, _ = part.shape
    spread = spread_matrix(cols, proj.shape[1])
    frames = (lambda i: two_frame[i], lambda i: act_two[i])
    for k in range(0, n_out, 2):
        if k % 4 == 0:
            wide = jnp.dot(spread, jnp.concatenate([proj[k // 2], proj[k // 2 + 1]], axis=1), preferred_element_type=F32)
        base = wide[:, k % 4 * 64 : k % 4 * 64 + 128] + bias[...]
        for h, v in enumerate(conv_rows(frames, (0, 2), weight, k, sums, k // 2 % 2)):
            part[k + h] = v[B : B + cols] + base


def middle_two_kernel(middle, part, weight, out, sums, done, sems):
    n_out, cols, _ = done.shape
    copies = []
    for k in range(0, n_out, 2):
        for h, v in enumerate(conv_rows((lambda i: middle[i],), (1,), weight, k, sums, k // 2 % 2)):
            done[k + h] = (part[k + h] + v[B : B + cols]).astype(BF)
        copies.append(pltpu.make_async_copy(done.at[k : k + 2], out.at[k : k + 2], sems.at[k // 2]))
        copies[-1].start()
    for c in copies:
        c.wait()


def exchange(x, axis, first):
    pairs = [(i, i + 1) for i in range(first, lax.axis_size(axis) - 1, 2)]
    return lax.ppermute(x, axis, pairs + [(j, i) for i, j in pairs])


def swap(x):
    return lax.ppermute(x, "frm", [(0, 1), (1, 0)])


def program(latent, proj_weight, proj_bias, cache_one, cache_two, conv_one, bias_one, conv_two, bias_two):
    latent, one, two = latent[0], cache_one[0], cache_two[0]
    rows, cols, ch = one.shape
    crows, ccols, lch = latent.shape
    span = cols + 2 * B
    n_edge = (2 * rows + crows) * B
    col_shape = (2 * rows + crows, E, ch)
    n_row = 3 * cols + ccols
    sums = pltpu.VMEM((4, span + 16, 2 * ch), F32)
    proj, act, row_0, row_1, col_0, col_1, b_one, b_two = call(
        first_kernel,
        [
            ((crows, ccols, ch), BF),
            ((crows, ccols, ch), BF),
            ((n_row, ch), BF),
            ((n_row, ch), BF),
            (col_shape, BF),
            (col_shape, BF),
            ((1, ch), F32),
            ((1, ch), F32),
        ],
        [HBM] * 7,
        scratch=[
            pltpu.VMEM((crows, ccols, lch), BF),
            pltpu.VMEM((lch, ch), BF),
            pltpu.VMEM((1, ch), F32),
            pltpu.SemaphoreType.DMA((15,)),
        ],
        flops=10**8,
        nbytes=2 * 10**6,
        limit=24,
    )(latent, proj_weight, proj_bias.reshape(1, ch), one, two, bias_one.reshape(1, ch), bias_two.reshape(1, ch))
    got_1 = exchange(col_1, "col", 1)
    got_0 = exchange(col_0, "col", 0)
    row_1 = exchange(row_1, "row", 1)
    row_0 = exchange(row_0, "row", 0)
    third = 2 * 9 * ch * ch * rows * cols
    (act_up,) = call(fill_kernel, [((crows, cols, ch), BF)], [VMEM], flops=10**8, nbytes=10**6)(act)
    merged, act_edge, cor_0, cor_1 = call(
        functools.partial(corner_kernel, rows, crows),
        [((n_edge, ch), BF), ((crows * B, ch), BF), ((4 * B, ch), BF), ((4 * B, ch), BF)],
        [VMEM] * 2,
        flops=10**6,
        nbytes=2 * 10**5,
    )(got_0, got_1)
    cor_0 = exchange(cor_0, "row", 0)
    cor_1 = exchange(cor_1, "row", 1)
    (part_in,) = call(
        inner_kernel, [((rows - 2, span, ch), F32)], [VMEM] * 5, scratch=[sums], flops=2 * third, nbytes=4 * 10**6
    )(one, act_up, merged, act_edge, conv_one)
    cache_border, act_border, send = call(
        border_kernel,
        [((4, span, ch), BF), ((2, span, ch), BF), ((rows + 4, span, ch), BF)],
        [VMEM] * 8,
        flops=10**8,
        nbytes=4 * 10**6,
    )(one, act_up, merged, act_edge, row_0, row_1, cor_0, cor_1)
    middle = swap(send)
    part_out, two_frame = call(
        functools.partial(outer_kernel, first=rows + crows),
        [((4, span, ch), F32), ((rows + 2, span, ch), BF)],
        [VMEM] * 12,
        scratch=[sums],
        flops=third,
        nbytes=4 * 10**6,
    )(one, act_up, merged, act_edge, cache_border, act_border, conv_one, two, row_0, row_1, cor_0, cor_1)
    act_two, send_two = call(
        middle_kernel,
        [((rows + 2, span, ch), BF)] * 2,
        [VMEM] * 6,
        scratch=[pltpu.VMEM((rows + 4, span, 2 * ch), BF)],
        flops=third,
        nbytes=6 * 10**6,
    )(middle, part_in, part_out, conv_one, b_one, two_frame)
    middle_two = swap(send_two)
    (part_two,) = call(
        own_two_kernel, [((rows, cols, ch), F32)], [VMEM] * 5, scratch=[sums], flops=2 * third, nbytes=6 * 10**6
    )(two_frame, act_two, conv_two, proj, b_two)
    (decoded,) = call(
        middle_two_kernel,
        [((rows, cols, ch), BF)],
        [VMEM] * 3,
        scratch=[sums, pltpu.VMEM((rows, cols, ch), BF), pltpu.SemaphoreType.DMA((rows // 2,))],
        out_specs=[HBM],
        flops=third,
        nbytes=6 * 10**6,
    )(middle_two, part_two, conv_two)
    return decoded[None]


def solution(mesh):
    placed = (
        P(("grp", "frm"), "row", "col", None),
        P(),
        P(),
        P(("grp", "frm"), "row", "col", None),
        P(("grp", "frm"), "row", "col", None),
        P(),
        P(),
        P(),
        P(),
    )
    return jax.shard_map(
        program,
        mesh=mesh,
        in_specs=placed,
        out_specs=P(("grp", "frm"), "row", "col", None),
        check_vma=False,
    )
```

```python
import functools

import jax
import jax.numpy as jnp
from jax import lax
from jax.experimental import pallas as pl
from jax.experimental.pallas import tpu as pltpu
from jax.sharding import PartitionSpec as P

B = 16
E = B // 2
BF = jnp.bfloat16
F32 = jnp.float32
VMEM = pl.BlockSpec(memory_space=pltpu.VMEM)
HBM = pl.BlockSpec(memory_space=pltpu.HBM)


def call(body, outs, specs, scratch=(), flops=0, nbytes=0, limit=24, out_specs=None):
    run = pl.pallas_call(
        body,
        out_shape=[jax.ShapeDtypeStruct(s, d) for s, d in outs],
        in_specs=specs,
        out_specs=out_specs or [VMEM] * len(outs),
        scratch_shapes=list(scratch),
        cost_estimate=pl.CostEstimate(flops=flops, bytes_accessed=nbytes, transcendentals=0),
        compiler_params=pltpu.CompilerParams(vmem_limit_bytes=int(limit * 1024 * 1024)),
    )
    held = lambda v, spec: pltpu.with_memory_space_constraint(v, pltpu.HBM) if spec is HBM else v
    return lambda *args: run(*(held(v, spec) for v, spec in zip(args, specs, strict=True)))


def silu(v):
    return v / (1.0 + jnp.exp(-v))


def low_half():
    return lax.broadcasted_iota(jnp.int32, (B, 128), 0) < B // 2


def spread_matrix(cols, ccols):
    fine = lax.broadcasted_iota(jnp.int32, (cols, ccols), 0)
    return (fine // 2 == lax.broadcasted_iota(jnp.int32, (cols, ccols), 1)).astype(F32).astype(BF)


def even(axis):
    return lax.rem(lax.axis_index(axis), 2) == 0


def pick(axis, high, low, step=1):
    start = jnp.where(even(axis), high, low)
    return pl.multiple_of(start, step) if step > 1 else start


def project(x, weight, bias):
    p = (jnp.dot(x, weight, preferred_element_type=F32) + bias).astype(BF)
    return p, silu(p.astype(F32)).astype(BF)


def first_kernel(
    latent, weight, bias, one, two, bias_one, bias_two,
    col_0, col_1, weight_v, bias_v, b_one, b_two,
    latent_v, sems,
):
    rows, cols, _ = one.shape
    crows, ccols, _ = latent.shape
    copies = [(weight, weight_v), (bias, bias_v)]
    sends = ((col_0, False), (col_1, True))
    for n, (col_s, flip) in enumerate(sends):
        lo, hi = (ccols - E, 0) if flip else (0, ccols - E)
        copies.append((latent.at[:, pl.ds(pick("col", hi, lo, E), E)], latent_v.at[n]))
    n_first = len(copies)
    for col_s, flip in sends:
        lo, hi = (cols - E, 0) if flip else (0, cols - E)
        c = pl.ds(pick("col", hi, lo, E), E)
        copies.append((one.at[:, c], col_s.at[0:rows]))
        copies.append((two.at[:, c], col_s.at[rows + crows :]))
    copies.append((bias_one, b_one))
    copies.append((bias_two, b_two))
    started = [pltpu.make_async_copy(s, d, sems.at[i]) for i, (s, d) in enumerate(copies)]
    for c in started:
        c.start()
    for c in started[:n_first]:
        c.wait()
    edges = jnp.concatenate([latent_v[n, i] for n in range(2) for i in range(crows)], axis=0)
    _, a = project(edges, weight_v[...], bias_v[...])
    for n, (col_s, _) in enumerate(sends):
        for i in range(crows):
            o = (n * crows + i) * E
            col_s[rows + i] = a[o : o + E]
    for c in started[n_first:]:
        c.wait()


def rows_kernel(latent, weight, bias, one, two, proj, act, row_0, row_1):
    rows, cols, _ = one.shape
    crows, ccols, _ = latent.shape
    for i in range(crows):
        proj[i], act[i] = project(latent[i], weight[...], bias[...])
    t0 = 2 * cols + ccols
    for row_s, flip in ((row_0, False), (row_1, True)):
        lo, hi = (rows - 2, 0) if flip else (0, rows - 2)
        r = pick("row", hi, lo)
        for k in range(2):
            row_s[k * cols : (k + 1) * cols, :] = one[r + k]
        lo, hi = (crows - 1, 0) if flip else (0, crows - 1)
        row_s[2 * cols : t0, :] = act[pick("row", hi, lo)]
        lo, hi = (rows - 1, 0) if flip else (0, rows - 1)
        row_s[t0:, :] = two[pick("row", hi, lo)]


def corner_kernel(rows, crows, got_0, got_1, merged, act_edge, cor_0, cor_1):
    is_even = even("col")
    for i in range(2 * rows + crows):
        x, y = (g[i].astype(F32) for g in (got_0, got_1))
        both = jnp.concatenate([jnp.where(is_even, x, y), jnp.where(is_even, y, x)], axis=0)
        merged[i * B : (i + 1) * B, :] = both.astype(BF)
        if rows <= i < rows + crows:
            act_edge[(i - rows) * B : (i - rows + 1) * B, :] = spread_edge(both)
    lows = (0, 1, rows, rows + crows)
    highs = (rows - 2, rows - 1, rows + crows - 1, 2 * rows + crows - 1)
    for k, (lo, hi) in enumerate(zip(lows, highs)):
        s = slice(k * B, (k + 1) * B)
        cor_0[s, :] = merged[pl.ds(pick("row", hi * B, lo * B, B), B), :]
        cor_1[s, :] = merged[pl.ds(pick("row", lo * B, hi * B, B), B), :]


def block(ref, i):
    return ref[i * B : (i + 1) * B, :].astype(F32)


def spread_edge(m):
    return jnp.where(
        low_half(), jnp.broadcast_to(m[0:1], (B, 128)), jnp.broadcast_to(m[B - 1 : B], (B, 128))
    ).astype(BF)


def put_row(dst, i, inside, edges):
    cols = dst.shape[1] - 2 * B
    dst[i, 0:B, :] = edges
    dst[i, B : B + cols, :] = inside
    dst[i, B + cols :, :] = edges


def conv_rows(frames, steps, weight, k, sums, slot):
    span = sums.shape[1] - 16
    w01, w2 = [], []
    zero = jnp.zeros(weight.shape[3:], BF)
    for a in steps:
        for p in range(4):
            if p < 3:
                w01.append(jnp.concatenate([weight[a, p, 0], weight[a, p, 1]], axis=1))
            w2.append(jnp.concatenate([weight[a, p, 2] if p < 3 else zero, weight[a, p - 1, 2] if p else zero], axis=1))
    w01, w2 = jnp.concatenate(w01, axis=0), jnp.concatenate(w2, axis=0)
    lhs = jnp.concatenate([f(k + p) for f in frames for p in range(4)], axis=1)
    y2 = jnp.dot(lhs, w2, preferred_element_type=F32)
    results = []
    for h in range(2):
        lhs = jnp.concatenate([f(k + h + p) for f in frames for p in range(3)], axis=1)
        y01 = jnp.dot(lhs, w01, preferred_element_type=F32)
        s = 2 * slot + h
        sums[s, 8 : 8 + span, 0:128] = y01[:, 0:128]
        sums[s, 8 : 8 + span, 128:256] = y2[:, h * 128 : (h + 1) * 128]
        results.append(sums[s, 7 : 7 + span, 0:128] + y01[:, 128:256] + sums[s, 9 : 9 + span, 128:256])
    return results


def shift_rows(frame, rows, moved):
    span = moved.shape[1]
    for i in rows:
        x = frame(i).astype(F32)
        moved[i, :, 0:128] = pltpu.roll(x, 1, 0).astype(BF)
        moved[i, :, 128:256] = pltpu.roll(x, span - 1, 0).astype(BF)


def conv_pair(frame, moved, step, weight, k):
    lhs, rhs = [], []
    zero = jnp.zeros(weight.shape[3:], BF)
    for p in range(4):
        lhs += [moved[k + p], frame(k + p)]
        for q in (0, 2, 1):
            first = weight[step, p, q] if p < 3 else zero
            second = weight[step, p - 1, q] if p else zero
            rhs.append(jnp.concatenate([first, second], axis=1))
    y = jnp.dot(jnp.concatenate(lhs, axis=1), jnp.concatenate(rhs, axis=0), preferred_element_type=F32)
    return y[:, 0:128], y[:, 128:256]


def joined(core, border):
    core, n = core
    return lambda i: border(i) if i < 2 else core(i - 2) if i < n + 2 else border(i - n)


def framed(tile, edges, first=0, each=1):
    def row(i):
        i = i // each
        e = edges[first + i * B : first + (i + 1) * B, :]
        return jnp.concatenate([e, tile[i], e], axis=0)

    return row, tile.shape[0] * each


def fill_kernel(act, act_up):
    crows, cols, _ = act_up.shape
    ccols = act.shape[1]
    spread = spread_matrix(cols, ccols)
    for m in range(0, crows, 2):
        wide = jnp.dot(spread, jnp.concatenate([act[m], act[m + 1]], axis=1), preferred_element_type=F32).astype(BF)
        for h in range(2):
            act_up[m + h] = wide[:, h * 128 : (h + 1) * 128]


def inner_kernel(one, act_up, merged, act_edge, weight, part, sums):
    frames = [joined(f, None) for f in (framed(one, merged), framed(act_up, act_edge, each=2))]
    for n, k in enumerate(range(2, 2 + part.shape[0], 2)):
        for h, v in enumerate(conv_rows(frames, (0, 2), weight, k, sums, n % 2)):
            part[k - 2 + h] = v


def border_kernel(one, act_up, merged, act_edge, row_0, row_1, cor_0, cor_1, cache_border, act_border, send):
    rows, cols, _ = one.shape
    ccols = row_0.shape[0] - 3 * cols
    for even_row in (True, False):

        @pl.when(even("row") == even_row)
        def _(even_row=even_row):
            pairs = ((row_1, cor_1), (row_0, cor_0)) if even_row else ((row_0, cor_0), (row_1, cor_1))
            coarse = jnp.concatenate([row[2 * cols : 2 * cols + ccols, :] for row, _ in pairs], axis=1)
            wide = jnp.dot(spread_matrix(cols, ccols), coarse, preferred_element_type=F32).astype(BF)
            for h, (row, cor) in enumerate(pairs):
                for k in range(2):
                    put_row(cache_border, 2 * h + k, row[k * cols : (k + 1) * cols, :], cor[k * B : (k + 1) * B, :])
                put_row(act_border, h, wide[:, h * 128 : (h + 1) * 128], spread_edge(block(cor, 2)))

    lead = lax.axis_index("frm") == 0

    @pl.when(lead)
    def _():
        for i in range(4):
            send[i if i < 2 else rows + i] = act_border[i // 2]
        for i in range(rows):
            m = i // 2
            put_row(send, i + 2, act_up[m], act_edge[m * B : (m + 1) * B, :])

    @pl.when(jnp.logical_not(lead))
    def _():
        for i in range(4):
            send[i if i < 2 else rows + i] = cache_border[i]
        for i in range(rows):
            put_row(send, i + 2, one[i], merged[i * B : (i + 1) * B, :])


def outer_kernel(
    one, act_up, merged, act_edge, cache_border, act_border, weight, two, row_0, row_1, cor_0, cor_1,
    part, two_frame, sums, *, first,
):
    rows, cols, _ = two.shape
    frames = (
        joined(framed(one, merged), lambda i: cache_border[i]),
        joined(framed(act_up, act_edge, each=2), lambda i: act_border[i // 2]),
    )
    for n, k in enumerate((0, rows)):
        for h, v in enumerate(conv_rows(frames, (0, 2), weight, k, sums, n)):
            part[2 * n + h] = v
    t0 = row_0.shape[0] - cols
    for i in range(rows):
        put_row(two_frame, i + 1, two[i], merged[(first + i) * B : (first + i + 1) * B, :])
    for lead in (True, False):

        @pl.when(even("row") == lead)
        def _(lead=lead):
            put_row(two_frame, rows + 1 if lead else 0, row_0[t0:, :], cor_0[3 * B :, :])
            put_row(two_frame, 0 if lead else rows + 1, row_1[t0:, :], cor_1[3 * B :, :])


def finish_row(out, i, v, row, n_out):
    span = v.shape[0]
    t = lax.broadcasted_iota(jnp.int32, (B, 128), 0)
    keep_left = (t != B - 1) | (lax.axis_index("col") != 0)
    keep_right = (t != 0) | (lax.axis_index("col") != lax.axis_size("col") - 1)
    v = silu(v)
    if row == 0:
        v = jnp.where(lax.axis_index("row") != 0, v, 0.0)
    if row == n_out - 1:
        v = jnp.where(lax.axis_index("row") != lax.axis_size("row") - 1, v, 0.0)
    out[i, 0:B, :] = jnp.where(keep_left, v[0:B], 0.0).astype(BF)
    out[i, B : span - B, :] = v[B : span - B].astype(BF)
    out[i, span - B :, :] = jnp.where(keep_right, v[span - B :], 0.0).astype(BF)


def middle_kernel(middle, part_in, part_out, weight, bias, two_frame, out, send, moved):
    n_out, _, _ = out.shape
    row = lambda i: middle[i]
    for k in range(0, n_out, 2):
        shift_rows(row, range(k + 2 if k else 0, k + 4), moved)
        for h, v in enumerate(conv_pair(row, moved, 1, weight, k)):
            i = k + h
            part = part_in[i - 2] if 2 <= i < n_out - 2 else part_out[i if i < 2 else i - n_out + 4]
            finish_row(out, i, v + part + bias[...], i, n_out)
    for first, src in ((True, out), (False, two_frame)):

        @pl.when((lax.axis_index("frm") == 0) == first)
        def _(src=src):
            send[...] = src[...]


def own_two_kernel(two_frame, act_two, weight, proj, bias, part, sums):
    n_out, cols, _ = part.shape
    spread = spread_matrix(cols, proj.shape[1])
    frames = (lambda i: two_frame[i], lambda i: act_two[i])
    for k in range(0, n_out, 2):
        if k % 4 == 0:
            wide = jnp.dot(spread, jnp.concatenate([proj[k // 2], proj[k // 2 + 1]], axis=1), preferred_element_type=F32)
        base = wide[:, k % 4 * 64 : k % 4 * 64 + 128] + bias[...]
        for h, v in enumerate(conv_rows(frames, (0, 2), weight, k, sums, k // 2 % 2)):
            part[k + h] = v[B : B + cols] + base


def middle_two_kernel(middle, part, weight, out, sums, done, sems):
    n_out, cols, _ = done.shape
    copies = []
    for k in range(0, n_out, 2):
        for h, v in enumerate(conv_rows((lambda i: middle[i],), (1,), weight, k, sums, k // 2 % 2)):
            done[k + h] = (part[k + h] + v[B : B + cols]).astype(BF)
        copies.append(pltpu.make_async_copy(done.at[k : k + 2], out.at[k : k + 2], sems.at[k // 2]))
        copies[-1].start()
    for c in copies:
        c.wait()


def exchange(x, axis, first):
    pairs = [(i, i + 1) for i in range(first, lax.axis_size(axis) - 1, 2)]
    return lax.ppermute(x, axis, pairs + [(j, i) for i, j in pairs])


def swap(x):
    return lax.ppermute(x, "frm", [(0, 1), (1, 0)])


def program(latent, proj_weight, proj_bias, cache_one, cache_two, conv_one, bias_one, conv_two, bias_two):
    latent, one, two = latent[0], cache_one[0], cache_two[0]
    rows, cols, ch = one.shape
    crows, ccols, lch = latent.shape
    span = cols + 2 * B
    n_edge = (2 * rows + crows) * B
    col_shape = (2 * rows + crows, E, ch)
    n_row = 3 * cols + ccols
    sums = pltpu.VMEM((4, span + 16, 2 * ch), F32)
    col_0, col_1, weight_v, bias_v, b_one, b_two = call(
        first_kernel,
        [(col_shape, BF), (col_shape, BF), ((lch, ch), BF), ((1, ch), F32), ((1, ch), F32), ((1, ch), F32)],
        [HBM] * 7,
        scratch=[pltpu.VMEM((2, crows, E, lch), BF), pltpu.SemaphoreType.DMA((10,))],
        flops=10**7,
        nbytes=5 * 10**5,
    )(latent, proj_weight, proj_bias.reshape(1, ch), one, two, bias_one.reshape(1, ch), bias_two.reshape(1, ch))
    proj, act, row_0, row_1 = call(
        rows_kernel,
        [((crows, ccols, ch), BF), ((crows, ccols, ch), BF), ((n_row, ch), BF), ((n_row, ch), BF)],
        [VMEM] * 5,
        flops=10**8,
        nbytes=2 * 10**6,
    )(latent, weight_v, bias_v, one, two)
    got_1 = exchange(col_1, "col", 1)
    got_0 = exchange(col_0, "col", 0)
    row_1 = exchange(row_1, "row", 1)
    row_0 = exchange(row_0, "row", 0)
    third = 2 * 9 * ch * ch * rows * cols
    (act_up,) = call(fill_kernel, [((crows, cols, ch), BF)], [VMEM], flops=10**8, nbytes=10**6)(act)
    merged, act_edge, cor_0, cor_1 = call(
        functools.partial(corner_kernel, rows, crows),
        [((n_edge, ch), BF), ((crows * B, ch), BF), ((4 * B, ch), BF), ((4 * B, ch), BF)],
        [VMEM] * 2,
        flops=10**6,
        nbytes=2 * 10**5,
    )(got_0, got_1)
    cor_0 = exchange(cor_0, "row", 0)
    cor_1 = exchange(cor_1, "row", 1)
    (part_in,) = call(
        inner_kernel, [((rows - 2, span, ch), F32)], [VMEM] * 5, scratch=[sums], flops=2 * third, nbytes=4 * 10**6
    )(one, act_up, merged, act_edge, conv_one)
    cache_border, act_border, send = call(
        border_kernel,
        [((4, span, ch), BF), ((2, span, ch), BF), ((rows + 4, span, ch), BF)],
        [VMEM] * 8,
        flops=10**8,
        nbytes=4 * 10**6,
    )(one, act_up, merged, act_edge, row_0, row_1, cor_0, cor_1)
    middle = swap(send)
    part_out, two_frame = call(
        functools.partial(outer_kernel, first=rows + crows),
        [((4, span, ch), F32), ((rows + 2, span, ch), BF)],
        [VMEM] * 12,
        scratch=[sums],
        flops=third,
        nbytes=4 * 10**6,
    )(one, act_up, merged, act_edge, cache_border, act_border, conv_one, two, row_0, row_1, cor_0, cor_1)
    act_two, send_two = call(
        middle_kernel,
        [((rows + 2, span, ch), BF)] * 2,
        [VMEM] * 6,
        scratch=[pltpu.VMEM((rows + 4, span, 2 * ch), BF)],
        flops=third,
        nbytes=6 * 10**6,
    )(middle, part_in, part_out, conv_one, b_one, two_frame)
    middle_two = swap(send_two)
    (part_two,) = call(
        own_two_kernel, [((rows, cols, ch), F32)], [VMEM] * 5, scratch=[sums], flops=2 * third, nbytes=6 * 10**6
    )(two_frame, act_two, conv_two, proj, b_two)
    (decoded,) = call(
        middle_two_kernel,
        [((rows, cols, ch), BF)],
        [VMEM] * 3,
        scratch=[sums, pltpu.VMEM((rows, cols, ch), BF), pltpu.SemaphoreType.DMA((rows // 2,))],
        out_specs=[HBM],
        flops=third,
        nbytes=6 * 10**6,
    )(middle_two, part_two, conv_two)
    return decoded[None]


def solution(mesh):
    placed = (
        P(("grp", "frm"), "row", "col", None),
        P(),
        P(),
        P(("grp", "frm"), "row", "col", None),
        P(("grp", "frm"), "row", "col", None),
        P(),
        P(),
        P(),
        P(),
    )
    return jax.shard_map(
        program,
        mesh=mesh,
        in_specs=placed,
        out_specs=P(("grp", "frm"), "row", "col", None),
        check_vma=False,
    )
```

```python
import functools

import jax
import jax.numpy as jnp
from jax import lax
from jax.experimental import pallas as pl
from jax.experimental.pallas import tpu as pltpu
from jax.sharding import PartitionSpec as P

B = 16
E = B // 2
BF = jnp.bfloat16
F32 = jnp.float32
VMEM = pl.BlockSpec(memory_space=pltpu.VMEM)
HBM = pl.BlockSpec(memory_space=pltpu.HBM)


def call(body, outs, specs, scratch=(), flops=0, nbytes=0, limit=24, out_specs=None):
    run = pl.pallas_call(
        body,
        out_shape=[jax.ShapeDtypeStruct(s, d) for s, d in outs],
        in_specs=specs,
        out_specs=out_specs or [VMEM] * len(outs),
        scratch_shapes=list(scratch),
        cost_estimate=pl.CostEstimate(flops=flops, bytes_accessed=nbytes, transcendentals=0),
        compiler_params=pltpu.CompilerParams(vmem_limit_bytes=int(limit * 1024 * 1024)),
    )
    held = lambda v, spec: pltpu.with_memory_space_constraint(v, pltpu.HBM) if spec is HBM else v
    return lambda *args: run(*(held(v, spec) for v, spec in zip(args, specs, strict=True)))


def silu(v):
    return v / (1.0 + jnp.exp(-v))


def low_half():
    return lax.broadcasted_iota(jnp.int32, (B, 128), 0) < B // 2


def spread_matrix(cols, ccols):
    fine = lax.broadcasted_iota(jnp.int32, (cols, ccols), 0)
    return (fine // 2 == lax.broadcasted_iota(jnp.int32, (cols, ccols), 1)).astype(F32).astype(BF)


def even(axis):
    return lax.rem(lax.axis_index(axis), 2) == 0


def pick(axis, high, low, step=1):
    start = jnp.where(even(axis), high, low)
    return pl.multiple_of(start, step) if step > 1 else start


def project(x, weight, bias):
    p = (jnp.dot(x, weight, preferred_element_type=F32) + bias).astype(BF)
    return p, silu(p.astype(F32)).astype(BF)


def first_kernel(
    latent, weight, bias, one, two, bias_one, bias_two,
    col_0, col_1, weight_v, bias_v, b_one, b_two,
    latent_v, sems,
):
    rows, cols, _ = one.shape
    crows, ccols, _ = latent.shape
    copies = [(weight, weight_v), (bias, bias_v)]
    sends = ((col_0, False), (col_1, True))
    for n, (col_s, flip) in enumerate(sends):
        lo, hi = (ccols - E, 0) if flip else (0, ccols - E)
        copies.append((latent.at[:, pl.ds(pick("col", hi, lo, E), E)], latent_v.at[n]))
    n_first = len(copies)
    for col_s, flip in sends:
        lo, hi = (cols - E, 0) if flip else (0, cols - E)
        c = pl.ds(pick("col", hi, lo, E), E)
        copies.append((one.at[:, c], col_s.at[0:rows]))
        copies.append((two.at[:, c], col_s.at[rows + crows :]))
    copies.append((bias_one, b_one))
    copies.append((bias_two, b_two))
    started = [pltpu.make_async_copy(s, d, sems.at[i]) for i, (s, d) in enumerate(copies)]
    for c in started:
        c.start()
    for c in started[:n_first]:
        c.wait()
    edges = jnp.concatenate([latent_v[n, i] for n in range(2) for i in range(crows)], axis=0)
    _, a = project(edges, weight_v[...], bias_v[...])
    for n, (col_s, _) in enumerate(sends):
        for i in range(crows):
            o = (n * crows + i) * E
            col_s[rows + i] = a[o : o + E]
    for c in started[n_first:]:
        c.wait()


def rows_kernel(latent, weight, bias, one, two, proj, act, row_0, row_1):
    rows, cols, _ = one.shape
    crows, ccols, _ = latent.shape
    for i in range(crows):
        proj[i], act[i] = project(latent[i], weight[...], bias[...])
    t0 = 2 * cols + ccols
    for row_s, flip in ((row_0, False), (row_1, True)):
        lo, hi = (rows - 2, 0) if flip else (0, rows - 2)
        r = pick("row", hi, lo)
        for k in range(2):
            row_s[k * cols : (k + 1) * cols, :] = one[r + k]
        lo, hi = (crows - 1, 0) if flip else (0, crows - 1)
        row_s[2 * cols : t0, :] = act[pick("row", hi, lo)]
        lo, hi = (rows - 1, 0) if flip else (0, rows - 1)
        row_s[t0:, :] = two[pick("row", hi, lo)]


def corner_kernel(rows, crows, got_0, got_1, merged, act_edge, cor_0, cor_1):
    is_even = even("col")
    for i in range(2 * rows + crows):
        x, y = (g[i].astype(F32) for g in (got_0, got_1))
        both = jnp.concatenate([jnp.where(is_even, x, y), jnp.where(is_even, y, x)], axis=0)
        merged[i * B : (i + 1) * B, :] = both.astype(BF)
        if rows <= i < rows + crows:
            act_edge[(i - rows) * B : (i - rows + 1) * B, :] = spread_edge(both)
    lows = (0, 1, rows, rows + crows)
    highs = (rows - 2, rows - 1, rows + crows - 1, 2 * rows + crows - 1)
    for k, (lo, hi) in enumerate(zip(lows, highs)):
        s = slice(k * B, (k + 1) * B)
        cor_0[s, :] = merged[pl.ds(pick("row", hi * B, lo * B, B), B), :]
        cor_1[s, :] = merged[pl.ds(pick("row", lo * B, hi * B, B), B), :]


def block(ref, i):
    return ref[i * B : (i + 1) * B, :].astype(F32)


def spread_edge(m):
    return jnp.where(
        low_half(), jnp.broadcast_to(m[0:1], (B, 128)), jnp.broadcast_to(m[B - 1 : B], (B, 128))
    ).astype(BF)


def put_row(dst, i, inside, edges):
    cols = dst.shape[1] - 2 * B
    dst[i, 0:B, :] = edges
    dst[i, B : B + cols, :] = inside
    dst[i, B + cols :, :] = edges


def conv_rows(frames, steps, weight, k, sums, slot):
    span = sums.shape[1] - 16
    w01, w2 = [], []
    zero = jnp.zeros(weight.shape[3:], BF)
    for a in steps:
        for p in range(4):
            if p < 3:
                w01.append(jnp.concatenate([weight[a, p, 0], weight[a, p, 1]], axis=1))
            w2.append(jnp.concatenate([weight[a, p, 2] if p < 3 else zero, weight[a, p - 1, 2] if p else zero], axis=1))
    w01, w2 = jnp.concatenate(w01, axis=0), jnp.concatenate(w2, axis=0)
    lhs = jnp.concatenate([f(k + p) for f in frames for p in range(4)], axis=1)
    y2 = jnp.dot(lhs, w2, preferred_element_type=F32)
    results = []
    for h in range(2):
        lhs = jnp.concatenate([f(k + h + p) for f in frames for p in range(3)], axis=1)
        y01 = jnp.dot(lhs, w01, preferred_element_type=F32)
        s = 2 * slot + h
        sums[s, 8 : 8 + span, 0:128] = y01[:, 0:128]
        sums[s, 8 : 8 + span, 128:256] = y2[:, h * 128 : (h + 1) * 128]
        results.append(sums[s, 7 : 7 + span, 0:128] + y01[:, 128:256] + sums[s, 9 : 9 + span, 128:256])
    return results


def shift_rows(frame, rows, moved):
    span = moved.shape[1]
    for i in rows:
        x = frame(i).astype(F32)
        moved[i, :, 0:128] = pltpu.roll(x, 1, 0).astype(BF)
        moved[i, :, 128:256] = pltpu.roll(x, span - 1, 0).astype(BF)


def conv_pair(frame, moved, step, weight, k):
    lhs, rhs = [], []
    zero = jnp.zeros(weight.shape[3:], BF)
    for p in range(4):
        lhs += [moved[k + p], frame(k + p)]
        for q in (0, 2, 1):
            first = weight[step, p, q] if p < 3 else zero
            second = weight[step, p - 1, q] if p else zero
            rhs.append(jnp.concatenate([first, second], axis=1))
    y = jnp.dot(jnp.concatenate(lhs, axis=1), jnp.concatenate(rhs, axis=0), preferred_element_type=F32)
    return y[:, 0:128], y[:, 128:256]


def joined(core, border):
    core, n = core
    return lambda i: border(i) if i < 2 else core(i - 2) if i < n + 2 else border(i - n)


def framed(tile, edges, first=0, each=1):
    def row(i):
        i = i // each
        e = edges[first + i * B : first + (i + 1) * B, :]
        return jnp.concatenate([e, tile[i], e], axis=0)

    return row, tile.shape[0] * each


def fill_kernel(act, act_up):
    crows, cols, _ = act_up.shape
    ccols = act.shape[1]
    spread = spread_matrix(cols, ccols)
    for m in range(0, crows, 2):
        wide = jnp.dot(spread, jnp.concatenate([act[m], act[m + 1]], axis=1), preferred_element_type=F32).astype(BF)
        for h in range(2):
            act_up[m + h] = wide[:, h * 128 : (h + 1) * 128]


def inner_kernel(one, act_up, merged, act_edge, weight, part, sums):
    frames = [joined(f, None) for f in (framed(one, merged), framed(act_up, act_edge, each=2))]
    for n, k in enumerate(range(2, 2 + part.shape[0], 2)):
        for h, v in enumerate(conv_rows(frames, (0, 2), weight, k, sums, n % 2)):
            part[k - 2 + h] = v


def border_kernel(one, act_up, merged, act_edge, row_0, row_1, cor_0, cor_1, cache_border, act_border, send):
    rows, cols, _ = one.shape
    ccols = row_0.shape[0] - 3 * cols
    for even_row in (True, False):

        @pl.when(even("row") == even_row)
        def _(even_row=even_row):
            pairs = ((row_1, cor_1), (row_0, cor_0)) if even_row else ((row_0, cor_0), (row_1, cor_1))
            coarse = jnp.concatenate([row[2 * cols : 2 * cols + ccols, :] for row, _ in pairs], axis=1)
            wide = jnp.dot(spread_matrix(cols, ccols), coarse, preferred_element_type=F32).astype(BF)
            for h, (row, cor) in enumerate(pairs):
                for k in range(2):
                    put_row(cache_border, 2 * h + k, row[k * cols : (k + 1) * cols, :], cor[k * B : (k + 1) * B, :])
                put_row(act_border, h, wide[:, h * 128 : (h + 1) * 128], spread_edge(block(cor, 2)))

    lead = lax.axis_index("frm") == 0
    for i in range(4):
        send[i if i < 2 else rows + i] = jnp.where(lead, act_border[i // 2], cache_border[i])
    for i in range(rows):
        m = i // 2
        edges = jnp.where(lead, act_edge[m * B : (m + 1) * B, :], merged[i * B : (i + 1) * B, :])
        put_row(send, i + 2, jnp.where(lead, act_up[m], one[i]), edges)


def outer_kernel(
    one, act_up, merged, act_edge, cache_border, act_border, weight, two, row_0, row_1, cor_0, cor_1,
    part, two_frame, sums, *, first,
):
    rows, cols, _ = two.shape
    frames = (
        joined(framed(one, merged), lambda i: cache_border[i]),
        joined(framed(act_up, act_edge, each=2), lambda i: act_border[i // 2]),
    )
    for n, k in enumerate((0, rows)):
        for h, v in enumerate(conv_rows(frames, (0, 2), weight, k, sums, n)):
            part[2 * n + h] = v
    t0 = row_0.shape[0] - cols
    for i in range(rows):
        put_row(two_frame, i + 1, two[i], merged[(first + i) * B : (first + i + 1) * B, :])
    for lead in (True, False):

        @pl.when(even("row") == lead)
        def _(lead=lead):
            put_row(two_frame, rows + 1 if lead else 0, row_0[t0:, :], cor_0[3 * B :, :])
            put_row(two_frame, 0 if lead else rows + 1, row_1[t0:, :], cor_1[3 * B :, :])


def finish_row(out, i, v, row, n_out):
    span = v.shape[0]
    t = lax.broadcasted_iota(jnp.int32, (B, 128), 0)
    keep_left = (t != B - 1) | (lax.axis_index("col") != 0)
    keep_right = (t != 0) | (lax.axis_index("col") != lax.axis_size("col") - 1)
    v = silu(v)
    if row == 0:
        v = jnp.where(lax.axis_index("row") != 0, v, 0.0)
    if row == n_out - 1:
        v = jnp.where(lax.axis_index("row") != lax.axis_size("row") - 1, v, 0.0)
    out[i, 0:B, :] = jnp.where(keep_left, v[0:B], 0.0).astype(BF)
    out[i, B : span - B, :] = v[B : span - B].astype(BF)
    out[i, span - B :, :] = jnp.where(keep_right, v[span - B :], 0.0).astype(BF)


def middle_kernel(middle, part_in, part_out, weight, bias, two_frame, out, send, moved):
    n_out, _, _ = out.shape
    row = lambda i: middle[i]
    for k in range(0, n_out, 2):
        shift_rows(row, range(k + 2 if k else 0, k + 4), moved)
        for h, v in enumerate(conv_pair(row, moved, 1, weight, k)):
            i = k + h
            part = part_in[i - 2] if 2 <= i < n_out - 2 else part_out[i if i < 2 else i - n_out + 4]
            finish_row(out, i, v + part + bias[...], i, n_out)
    for first, src in ((True, out), (False, two_frame)):

        @pl.when((lax.axis_index("frm") == 0) == first)
        def _(src=src):
            send[...] = src[...]


def own_two_kernel(two_frame, act_two, weight, proj, bias, part, sums):
    n_out, cols, _ = part.shape
    spread = spread_matrix(cols, proj.shape[1])
    frames = (lambda i: two_frame[i], lambda i: act_two[i])
    for k in range(0, n_out, 2):
        if k % 4 == 0:
            wide = jnp.dot(spread, jnp.concatenate([proj[k // 2], proj[k // 2 + 1]], axis=1), preferred_element_type=F32)
        base = wide[:, k % 4 * 64 : k % 4 * 64 + 128] + bias[...]
        for h, v in enumerate(conv_rows(frames, (0, 2), weight, k, sums, k // 2 % 2)):
            part[k + h] = v[B : B + cols] + base


def middle_two_kernel(middle, part, weight, out, sums, done, sems):
    n_out, cols, _ = done.shape
    copies = []
    for k in range(0, n_out, 2):
        for h, v in enumerate(conv_rows((lambda i: middle[i],), (1,), weight, k, sums, k // 2 % 2)):
            done[k + h] = (part[k + h] + v[B : B + cols]).astype(BF)
        copies.append(pltpu.make_async_copy(done.at[k : k + 2], out.at[k : k + 2], sems.at[k // 2]))
        copies[-1].start()
    for c in copies:
        c.wait()


def exchange(x, axis, first):
    pairs = [(i, i + 1) for i in range(first, lax.axis_size(axis) - 1, 2)]
    return lax.ppermute(x, axis, pairs + [(j, i) for i, j in pairs])


def swap(x):
    return lax.ppermute(x, "frm", [(0, 1), (1, 0)])


def program(latent, proj_weight, proj_bias, cache_one, cache_two, conv_one, bias_one, conv_two, bias_two):
    latent, one, two = latent[0], cache_one[0], cache_two[0]
    rows, cols, ch = one.shape
    crows, ccols, lch = latent.shape
    span = cols + 2 * B
    n_edge = (2 * rows + crows) * B
    col_shape = (2 * rows + crows, E, ch)
    n_row = 3 * cols + ccols
    sums = pltpu.VMEM((4, span + 16, 2 * ch), F32)
    col_0, col_1, weight_v, bias_v, b_one, b_two = call(
        first_kernel,
        [(col_shape, BF), (col_shape, BF), ((lch, ch), BF), ((1, ch), F32), ((1, ch), F32), ((1, ch), F32)],
        [HBM] * 7,
        scratch=[pltpu.VMEM((2, crows, E, lch), BF), pltpu.SemaphoreType.DMA((10,))],
        flops=10**7,
        nbytes=5 * 10**5,
    )(latent, proj_weight, proj_bias.reshape(1, ch), one, two, bias_one.reshape(1, ch), bias_two.reshape(1, ch))
    proj, act, row_0, row_1 = call(
        rows_kernel,
        [((crows, ccols, ch), BF), ((crows, ccols, ch), BF), ((n_row, ch), BF), ((n_row, ch), BF)],
        [VMEM] * 5,
        flops=10**8,
        nbytes=2 * 10**6,
    )(latent, weight_v, bias_v, one, two)
    got_1 = exchange(col_1, "col", 1)
    got_0 = exchange(col_0, "col", 0)
    row_1 = exchange(row_1, "row", 1)
    row_0 = exchange(row_0, "row", 0)
    third = 2 * 9 * ch * ch * rows * cols
    (act_up,) = call(fill_kernel, [((crows, cols, ch), BF)], [VMEM], flops=10**8, nbytes=10**6)(act)
    merged, act_edge, cor_0, cor_1 = call(
        functools.partial(corner_kernel, rows, crows),
        [((n_edge, ch), BF), ((crows * B, ch), BF), ((4 * B, ch), BF), ((4 * B, ch), BF)],
        [VMEM] * 2,
        flops=10**6,
        nbytes=2 * 10**5,
    )(got_0, got_1)
    cor_0 = exchange(cor_0, "row", 0)
    cor_1 = exchange(cor_1, "row", 1)
    (part_in,) = call(
        inner_kernel, [((rows - 2, span, ch), F32)], [VMEM] * 5, scratch=[sums], flops=2 * third, nbytes=4 * 10**6
    )(one, act_up, merged, act_edge, conv_one)
    cache_border, act_border, send = call(
        border_kernel,
        [((4, span, ch), BF), ((2, span, ch), BF), ((rows + 4, span, ch), BF)],
        [VMEM] * 8,
        flops=10**8,
        nbytes=4 * 10**6,
    )(one, act_up, merged, act_edge, row_0, row_1, cor_0, cor_1)
    middle = swap(send)
    part_out, two_frame = call(
        functools.partial(outer_kernel, first=rows + crows),
        [((4, span, ch), F32), ((rows + 2, span, ch), BF)],
        [VMEM] * 12,
        scratch=[sums],
        flops=third,
        nbytes=4 * 10**6,
    )(one, act_up, merged, act_edge, cache_border, act_border, conv_one, two, row_0, row_1, cor_0, cor_1)
    act_two, send_two = call(
        middle_kernel,
        [((rows + 2, span, ch), BF)] * 2,
        [VMEM] * 6,
        scratch=[pltpu.VMEM((rows + 4, span, 2 * ch), BF)],
        flops=third,
        nbytes=6 * 10**6,
    )(middle, part_in, part_out, conv_one, b_one, two_frame)
    middle_two = swap(send_two)
    (part_two,) = call(
        own_two_kernel, [((rows, cols, ch), F32)], [VMEM] * 5, scratch=[sums], flops=2 * third, nbytes=6 * 10**6
    )(two_frame, act_two, conv_two, proj, b_two)
    (decoded,) = call(
        middle_two_kernel,
        [((rows, cols, ch), BF)],
        [VMEM] * 3,
        scratch=[sums, pltpu.VMEM((rows, cols, ch), BF), pltpu.SemaphoreType.DMA((rows // 2,))],
        out_specs=[HBM],
        flops=third,
        nbytes=6 * 10**6,
    )(middle_two, part_two, conv_two)
    return decoded[None]


def solution(mesh):
    placed = (
        P(("grp", "frm"), "row", "col", None),
        P(),
        P(),
        P(("grp", "frm"), "row", "col", None),
        P(("grp", "frm"), "row", "col", None),
        P(),
        P(),
        P(),
        P(),
    )
    return jax.shard_map(
        program,
        mesh=mesh,
        in_specs=placed,
        out_specs=P(("grp", "frm"), "row", "col", None),
        check_vma=False,
    )
```
